256 devices in a mesh: pop: 8 (over x_lo, y), dp: 32 (over z, x_hi, core).
Axes of the slice: x: 4 (x_hi: 2, x_lo: 2; x = x_hi * 2 + x_lo), y: 4, z: 8, core: 2. Of those that a mesh axis runs over, the one named last changes fastest.
Arguments:
- observations: bfloat16 [8, 16384, 256], P('pop', 'dp'), may hold values from -6 to 6
- returns: float32 [8, 16384], P('pop', 'dp'), may hold values from 0 to 2
- actions: int32 [8, 16384], P('pop', 'dp'), may hold values from 0 to 17
- w_input: bfloat16 [8, 256, 2048], P('pop', 'dp'), may hold values from -0.375 to 0.375
- w_middle: bfloat16 [8, 2048, 2048], P('pop', 'dp'), may hold values from -0.125 to 0.125
- w_head: bfloat16 [8, 2048, 18], P('pop', 'dp'), may hold values from -0.125 to 0.125
- log_rate: float32 [8], replicated, may hold values from 3 to 4
- copy_from: int32 [8], replicated, may hold values from 0 to 1, as said below
- perturb: int32 [8], replicated, may hold values from 0 to 2
Outputs:
- next_input: bfloat16 [8, 256, 2048], P('pop', 'dp')
- next_middle: bfloat16 [8, 2048, 2048], P('pop', 'dp')
- next_head: bfloat16 [8, 2048, 18], P('pop', 'dp')
- next_log_rate: float32 [8], P('pop')
- fitness: float32 [8], P('pop')
The draws below stay inside these ranges and needn't reach their ends.
Inputs may be any that keep to these rules, and one draw needn't show every extreme that they name: Some two members that lie 4 apart have copy_from 1.
All inputs are finite; a program needn't handle non-finite values.
Results may differ from the reference program's by a relative error of at most 0.014.
Values may be sent and summed in bfloat16 or wider, within the bound.
A program may use at most 128 MiB of HBM per device.

```python
import jax
import jax.numpy as jnp
from jax import lax

D = 2048
OBS = 256
ACT = 18
ROWS_DEV = 512
POP = 8
BATCH = 16384
N_DP = 32


def draw_copy_from(key, part):
    marks = jax.random.randint(jax.random.fold_in(key, 23), (POP,), 0, 2).astype(jnp.int32)
    turn = jax.random.randint(jax.random.fold_in(key, 41), (), 0, POP).astype(jnp.int32)
    members = jnp.arange(POP, dtype=jnp.int32)
    forced = (members == turn) | (members == (turn + POP // 2) % POP)
    return jnp.where(forced, 1, marks).astype(jnp.int32)


def with_ends(drawn, own_key, least, high):
    longest = drawn.shape.index(max(drawn.shape))
    spots = []
    for shift in (0, 1):
        where = [jax.random.randint(jax.random.fold_in(own_key, axis), (), 0, length) for axis, length in enumerate(drawn.shape)]
        where[longest] = (where[longest] + shift) % drawn.shape[longest]
        spots.append(tuple(where))
    return drawn.at[spots[0]].set(least).at[spots[1]].set(high)


def block_levels(own_key, shape, shards, smallest, largest):
    def one(axis_at, blocks):
        steps = jax.random.uniform(jax.random.fold_in(jax.random.fold_in(own_key, 6), axis_at), (blocks,), jnp.float32, smallest / len(shards), largest / len(shards))
        return jnp.repeat(jnp.exp(steps), shape[axis_at] // blocks).reshape((-1,) + (1,) * (len(shape) - axis_at - 1))

    gain = one(*shards[0])
    for cut in shards[1:]:
        gain = gain * one(*cut)
    return gain


def centred(own_key, dims, width, most, split=(), kind=jnp.bfloat16):
    loudness = block_levels(own_key, dims, split, -0.22, 0.18) if split else 1.0
    values = jax.random.normal(own_key, dims, jnp.float32) * width * loudness
    return jnp.minimum(jnp.maximum(values, -most), most).astype(kind)


def setup_inputs(seed: int = 0) -> dict:
    arg_keys = jax.random.split(jax.random.key(seed), 10)
    observations = centred(arg_keys[0], (POP, BATCH, OBS), 1.0, 6.0, ((0, 8), (1, 32)))
    returns = jnp.clip(2.0 * jax.random.uniform(arg_keys[1], (POP, BATCH), jnp.float32) ** block_levels(arg_keys[1], (POP, BATCH), ((0, 8), (1, 32)), -0.2, 0.2), 0.0, 2.0)
    actions = with_ends(jax.random.randint(arg_keys[2], (POP, BATCH), 0, ACT), jax.random.fold_in(arg_keys[2], 1), 0, ACT - 1).astype(jnp.int32)
    w_input = centred(arg_keys[3], (POP, OBS, D), OBS ** -0.5, 0.375, ((0, 8), (1, 32)))
    w_middle = centred(arg_keys[4], (POP, D, D), D ** -0.5, 0.125, ((0, 8), (1, 32)))
    w_head = centred(arg_keys[5], (POP, D, ACT), D ** -0.5, 0.125, ((0, 8), (1, 32)))
    log_rate = jnp.clip(jax.random.uniform(arg_keys[6], (POP,), jnp.float32, 3.0, 4.0), 3.0, 4.0)
    copy_from = draw_copy_from(jax.random.fold_in(arg_keys[9], 71), 0)
    perturb = with_ends(jax.random.randint(arg_keys[8], (POP,), 0, 3), jax.random.fold_in(arg_keys[8], 1), 0, 2).astype(jnp.int32)
    return dict(observations=observations, returns=returns, actions=actions, w_input=w_input, w_middle=w_middle, w_head=w_head, log_rate=log_rate, copy_from=copy_from, perturb=perturb)


CAP = 2.0


def silu_slope(pre):
    sig = jax.nn.sigmoid(pre)
    return sig * (1.0 + pre * (1.0 - sig))


def rounded(value):
    return lax.optimization_barrier(value.astype(jnp.bfloat16)).astype(jnp.float32)


def member_step(member):
    obs, gains, chosen, first, middle, head, rate = member
    pre1 = jnp.dot(obs, first, preferred_element_type=jnp.float32)
    hidden1 = jax.nn.silu(pre1).astype(jnp.bfloat16)
    pre2 = jnp.dot(hidden1, middle, preferred_element_type=jnp.float32)
    hidden2 = jax.nn.silu(pre2).astype(jnp.bfloat16)
    squash = jnp.tanh(jnp.dot(hidden2, head, preferred_element_type=jnp.float32) / CAP)
    logits = CAP * squash
    logp = logits - jnp.log(jnp.sum(jnp.exp(logits), axis=1, keepdims=True))
    onehot = (chosen[:, None] == lax.broadcasted_iota(jnp.int32, logits.shape, 1)).astype(jnp.float32)
    taken = jnp.sum(logp * onehot, axis=1)
    fitness = jnp.sum(gains * taken) / BATCH
    grad_raw = (-(gains / BATCH)[:, None] * (onehot - jnp.exp(logp)) * (1.0 - squash * squash)).astype(jnp.bfloat16)
    grad_pre2 = (jnp.dot(grad_raw, head.T, preferred_element_type=jnp.float32) * silu_slope(pre2)).astype(jnp.bfloat16)
    grad_pre1 = (jnp.dot(grad_pre2, middle.T, preferred_element_type=jnp.float32) * silu_slope(pre1)).astype(jnp.bfloat16)

    def add_block(carry, parts):
        obs_b, grad1_b, hid1_b, grad2_b, hid2_b, graw_b = parts
        total1, total2, total3 = carry
        total1 = total1 + rounded(jnp.dot(obs_b.T, grad1_b, preferred_element_type=jnp.float32))
        total2 = total2 + rounded(jnp.dot(hid1_b.T, grad2_b, preferred_element_type=jnp.float32))
        total3 = total3 + rounded(jnp.dot(hid2_b.T, graw_b, preferred_element_type=jnp.float32))
        return (total1, total2, total3), None

    blocks = tuple(part.reshape(N_DP, ROWS_DEV, part.shape[1]) for part in (obs, grad_pre1, hidden1, grad_pre2, hidden2, grad_raw))
    start = (jnp.zeros(first.shape, jnp.float32), jnp.zeros(middle.shape, jnp.float32), jnp.zeros(head.shape, jnp.float32))
    (grad_first, grad_middle, grad_head), unused = lax.scan(add_block, start, blocks)
    new_first = (first.astype(jnp.float32) - rate * grad_first).astype(jnp.bfloat16)
    new_middle = (middle.astype(jnp.float32) - rate * grad_middle).astype(jnp.bfloat16)
    new_head = (head.astype(jnp.float32) - rate * grad_head).astype(jnp.bfloat16)
    return new_first, new_middle, new_head, fitness


def reference(observations, returns, actions, w_input, w_middle, w_head, log_rate, copy_from, perturb):
    rates = jnp.exp(log_rate)
    new_first, new_middle, new_head, fitness = lax.map(member_step, (observations, returns, actions, w_input, w_middle, w_head, rates))
    flag = copy_from == 1
    next_input = jnp.where(flag[:, None, None], jnp.roll(new_first, 1, axis=0), new_first)
    next_middle = jnp.where(flag[:, None, None], jnp.roll(new_middle, 1, axis=0), new_middle)
    next_head = jnp.where(flag[:, None, None], jnp.roll(new_head, 1, axis=0), new_head)
    members = jnp.arange(POP, dtype=jnp.int32)
    source = jnp.where(flag, (members + POP - 1) % POP, members)
    offset = jnp.where(perturb == 0, -0.2, jnp.where(perturb == 1, 0.0, 0.2)).astype(jnp.float32)
    next_log_rate = log_rate[source] + offset
    return next_input, next_middle, next_head, next_log_rate, fitness
```

```python
import jax
import jax.numpy as jnp
from jax import lax
from jax.experimental import pallas as pl
from jax.experimental.pallas import tpu as pltpu
from jax.sharding import PartitionSpec as P

F32 = jnp.float32
BF16 = jnp.bfloat16
Z = 8
K = Z // 2
Q = 4
ROWS = 512
OBS = 256
D = 2048
QC = D // Q
BK = D // Z
ACT = 18
POP = 8
BATCH = ROWS * Z * Q
WI, WM, WH = 0, 1, 2
OB, QT, RAW, GR, DH, OUT = range(6)
RIGHT, LEFT = 0, 1


def nt(a, b):
    return lax.dot_general(a, b, (((1,), (1,)), ((), ())), preferred_element_type=F32)


def nn(a, b):
    return jnp.dot(a, b, preferred_element_type=F32)


def kernel(
    obs, ret, act, win, wmid, whead, lrate, copyf, pert,
    o_in, o_mid, o_head, o_rate, o_fit,
    ob, obT, wi, wh, wq, w1T, wT, h1, s1, p2, h2, g2, whq, whT,
    raw_s, raw_r, gr, dW, rss, rsb, dI, sib_s, sib_r, ris, rib, tin, xs, xr,
    dH, dHg, tH, nm, ym, om, ni, yi, nh, yh,
    ag_s, ag_r, gp_s, gp_r, xp_s, xp_r, sb_s, sb_r, dh_s, dh_r, rs_s, rs_r, ri_s, ri_r, y_s, y_r, loc,
):
    m = lax.axis_index("pop")
    d = lax.axis_index("dp")
    z = d // Q
    q = lax.rem(d, Q)
    h = q // 2
    c = lax.rem(q, 2)
    sib = {"dp": z * Q + h * 2 + (1 - c)}
    xpt = {"dp": z * Q + (1 - h) * 2 + c}
    side = [{"dp": lax.rem(z + 1, Z) * Q + q}, {"dp": lax.rem(z + Z - 1, Z) * Q + q}]
    after = {"pop": lax.rem(m + 1, POP)}
    before = {"pop": lax.rem(m + POP - 1, POP)}

    def mate(t):
        return lax.rem(q + t, Q)

    def mate_id(t):
        return {"dp": z * Q + mate(t)}

    def at(off):
        return lax.rem(z + off + Z, Z)

    def copy(src, dst, ss, rs, dev):
        return pltpu.make_async_remote_copy(
            src_ref=src, dst_ref=dst, send_sem=ss, recv_sem=rs, device_id=dev,
            device_id_type=pl.DeviceIdType.MESH,
        )

    fetch = [
        pltpu.make_async_copy(win, wi.at[z, h, c], loc.at[0]),
        pltpu.make_async_copy(wmid.at[:, pl.ds(pl.multiple_of(q * QC, QC), QC)], wq.at[z, q], loc.at[1]),
        pltpu.make_async_copy(whead, wh.at[z, h, c], loc.at[2]),
        pltpu.make_async_copy(obs, ob.at[q], loc.at[3]),
    ]
    for f in fetch:
        f.start()

    barrier = pltpu.get_barrier_semaphore()
    for dev in [mate_id(1), mate_id(2), mate_id(3), side[0], side[1], after, before]:
        pl.semaphore_signal(barrier, inc=1, device_id=dev, device_id_type=pl.DeviceIdType.MESH)
    pl.semaphore_wait(barrier, 7)

    xwi = copy(win, wi.at[z, h, c], xp_s.at[0], xp_r.at[0], xpt)
    xwi.start()
    xwh = copy(whead, wh.at[z, h, c], xp_s.at[1], xp_r.at[1], xpt)

    def quarter(t):
        p = mate(t)
        return copy(
            wmid.at[:, pl.ds(pl.multiple_of(p * QC, QC), QC)], wq.at[z, q], gp_s.at[QT, p], gp_r.at[QT, q], mate_id(t)
        )

    def sight(t):
        return copy(obs, ob.at[q], gp_s.at[OB, mate(t)], gp_r.at[OB, q], mate_id(t))

    def quarter_in(p):
        copy(wq.at[z, p], wq.at[z, p], gp_s.at[QT, p], gp_r.at[QT, p], sib).wait_recv()

    for t in (1, 2, 3):
        quarter(t).start()
    xwh.start()
    for t in (1, 2, 3):
        sight(t).start()

    def piece(kind, b, j):
        if kind == WI:
            return wi.at[b, j, c]
        if kind == WM:
            return wq.at[b, pl.ds(2 * j, 2)]
        return wh.at[b, j, c]

    def ag(kind, way, k, j):
        b = at(1 - k) if way == RIGHT else at(k - 1)
        ref = piece(kind, b, j)
        return copy(ref, ref, ag_s.at[kind, way, k - 1, j], ag_r.at[kind, way, k - 1, j], side[way])

    def ag_in(kind, way, k, j):
        b = at(-k) if way == RIGHT else at(k)
        ref = piece(kind, b, j)
        copy(ref, ref, ag_s.at[kind, way, k - 1, j], ag_r.at[kind, way, k - 1, j], side[way]).wait_recv()

    def put(kinds, k, j):
        for kind in kinds:
            for way in (RIGHT, LEFT):
                ag(kind, way, k, j).start()

    def take(kinds, k, j):
        for kind in kinds:
            for way in (RIGHT, LEFT):
                ag_in(kind, way, k, j)

    def take_last(kinds, k):
        for kind in kinds:
            ag_in(kind, RIGHT, k, 0)
            ag_in(kind, LEFT, k, 1)

    def put_last(kinds):
        for kind in kinds:
            ag(kind, RIGHT, K, 0).start()
            ag(kind, LEFT, K, 1).start()

    MID = (WM, WH)
    fetch[0].wait()
    put((WI,), 1, h)
    fetch[1].wait()
    fetch[2].wait()
    quarter_in(h * 2 + (1 - c))
    put(MID, 1, h)
    xwi.wait_recv()
    put((WI,), 1, 1 - h)
    take((WI,), 1, h)
    put((WI,), 2, h)
    quarter_in((1 - h) * 2)
    quarter_in((1 - h) * 2 + 1)
    xwh.wait_recv()
    put(MID, 1, 1 - h)
    take((WI,), 1, 1 - h)
    put((WI,), 2, 1 - h)

    fetch[3].wait()
    for t in (1, 2, 3):
        p = mate(t)
        copy(ob.at[p], ob.at[p], gp_s.at[OB, p], gp_r.at[OB, p], sib).wait_recv()

    def turn(i, _):
        x = ob[i].astype(F32)
        obT[:, pl.ds(pl.multiple_of(i * ROWS, ROWS), ROWS)] = jnp.transpose(x).astype(BF16)
        return 0

    lax.fori_loop(0, Q, turn, 0)
    take((WI,), 2, h)
    put((WI,), 3, h)
    take(MID, 1, h)
    put(MID, 2, h)
    take((WI,), 2, 1 - h)
    put((WI,), 3, 1 - h)
    take_last((WI,), 3)
    put_last((WI,))
    ag_in(WI, RIGHT, 3, 1)
    ag_in(WI, LEFT, 3, 0)
    take(MID, 1, 1 - h)
    put(MID, 2, 1 - h)
    take_last((WI,), K)

    def core_copy(ref, i):
        return copy(ref.at[:, :, c], ref.at[:, :, c], sb_s.at[i], sb_r.at[i], sib)

    def core_in(ref, i):
        copy(ref.at[:, :, 1 - c], ref.at[:, :, 1 - c], sb_s.at[i], sb_r.at[i], sib).wait_recv()

    core_copy(wi, 0).start()
    core_in(wi, 0)

    def turn_in(i, _):
        cols = pl.ds(pl.multiple_of(i * 256, 256), 256)
        x = wi[:, :, :, :, cols].astype(F32).reshape(OBS, 256)
        w1T[cols, :] = jnp.transpose(x).astype(BF16)
        return 0

    lax.fori_loop(0, D // 256, turn_in, 0)

    def unit(i, _):
        @pl.when(i == 1)
        def _():
            take(MID, 2, h)
            put(MID, 3, h)

        @pl.when(i == 2)
        def _():
            take(MID, 2, 1 - h)
            put(MID, 3, 1 - h)

        @pl.when(i == 4)
        def _():
            take_last(MID, 3)
            put_last(MID)

        @pl.when(i == 5)
        def _():
            for kind in MID:
                ag_in(kind, RIGHT, 3, 1)
                ag_in(kind, LEFT, 3, 0)

        @pl.when(i == 7)
        def _():
            take_last(MID, K)
            core_copy(wh, 1).start()

        b = at(((i + 1) // 2) * (2 * lax.rem(i + 1, 2) - 1))
        feats = pl.ds(pl.multiple_of(b * BK, BK), BK)
        wT[...] = jnp.transpose(wq[b].astype(F32).reshape(BK, QC)).astype(BF16)

        def tile(r, _):
            rows = pl.ds(pl.multiple_of(r * 256, 256), 256)
            v = nn(w1T[feats, :], obT[:, rows])
            s = 0.5 * jnp.tanh(0.5 * v) + 0.5
            hid = v * s
            hb = hid.astype(BF16)
            h1[feats, rows] = hb
            s1[feats, rows] = (s + hid * (1.0 - s)).astype(BF16)
            add = nn(wT[...], hb)
            p2[:, rows] = jnp.where(jnp.full(add.shape, i) == 0, add, p2[:, rows] + add)
            return 0

        lax.fori_loop(0, D // 256, tile, 0)
        return 0

    p2[...] = jnp.zeros_like(p2)
    lax.fori_loop(0, Z, unit, 0)

    core_in(wh, 1)
    whq[...] = jnp.zeros_like(whq)
    for i in range(2):
        whq[i * 256 : (i + 1) * 256, 0:ACT] = wh[2 * q + i].astype(F32).reshape(256, ACT)
    whT[...] = jnp.transpose(whq[...])[0:32, :].astype(BF16)

    def raw_out(p):
        return copy(raw_s.at[p], raw_r.at[q], gp_s.at[RAW, p], gp_r.at[RAW, q], {"dp": z * Q + p})

    for t in (2, 1, 3, 0):
        p = mate(t)
        rows = pl.ds(pl.multiple_of(p * ROWS, ROWS), ROWS)

        def forward2(i, _):
            cols = pl.ds(pl.multiple_of(p * ROWS + i * 128, 128), 128)
            v = p2[:, cols]
            s = 0.5 * jnp.tanh(0.5 * v) + 0.5
            hid = v * s
            h2[:, cols] = hid.astype(BF16)
            p2[:, cols] = s + hid * (1.0 - s)
            return 0

        lax.fori_loop(0, 4, forward2, 0)
        raw_s[p] = nn(whT[...], h2[:, rows])[0:24, :]
        if t:
            raw_out(p).start()
    raw = raw_s[q]
    for t in (2, 1, 3):
        p = mate(t)
        copy(raw_r.at[p], raw_r.at[p], gp_s.at[RAW, p], gp_r.at[RAW, p], sib).wait_recv()
        raw = raw + raw_r[p]
    at_act = lax.broadcasted_iota(jnp.int32, raw.shape, 0)
    squash = jnp.tanh(raw * 0.5)
    logits = 2.0 * squash
    e = jnp.where(at_act < ACT, jnp.exp(logits), 0.0)
    total = jnp.sum(e, axis=0, keepdims=True)
    logp = logits - jnp.log(total)
    onehot = jnp.where(at_act == act[...], 1.0, 0.0)
    gains = ret[...] * (1.0 / BATCH)
    term = gains * jnp.sum(logp * onehot, axis=0, keepdims=True)
    grad = -gains * (onehot - e / total) * (1.0 - squash * squash)
    high = term.astype(BF16).astype(F32)
    low = term - high
    grad = jnp.where(at_act < ACT, grad, jnp.where(at_act == ACT, high, jnp.where(at_act == ACT + 1, low, 0.0)))
    gr[q] = jnp.concatenate([grad, jnp.zeros((8, ROWS), F32)], axis=0).astype(BF16)

    def gr_out(t):
        return copy(gr.at[q], gr.at[q], gp_s.at[GR, mate(t)], gp_r.at[GR, q], mate_id(t))

    for t in (2, 1, 3):
        gr_out(t).start()
    wb = whq[...].astype(BF16)[:, 0:32]
    for t in (0, 1, 2, 3):
        p = mate(t)
        if t:
            copy(gr.at[p], gr.at[p], gp_s.at[GR, p], gp_r.at[GR, p], sib).wait_recv()
        rows = pl.ds(pl.multiple_of(p * ROWS, ROWS), ROWS)
        g2[:, rows] = (nn(wb, gr[p]) * p2[:, rows]).astype(BF16)

    def middle(i, _):
        b = at(K + ((i + 1) // 2) * (1 - 2 * lax.rem(i, 2)))
        feats = pl.ds(pl.multiple_of(b * BK, BK), BK)
        dW[b] = nt(h1[feats, :], g2[...]).reshape(Q, BK // Q, QC)
        return 0

    def rs_copy(way, k, p):
        return copy(
            rss.at[way, k - 1, p], rsb.at[way, k - 1, p], rs_s.at[way, k - 1, p], rs_r.at[way, k - 1, p], side[way]
        )

    def rs_in(way, k, p):
        copy(rsb.at[way, k, p], rsb.at[way, k, p], rs_s.at[way, k, p], rs_r.at[way, k, p], side[way]).wait_recv()
        return rsb[way, k, p].astype(F32)

    def rs_put(way, k, p, joined):
        v = dW[at(k if way == RIGHT else -k), p]
        if joined:
            v = v + rs_in(way, k, p)
        rss[way, k - 1, p] = v.astype(BF16)
        rs_copy(way, k, p).start()

    lax.fori_loop(0, 3, middle, 0)

    def rs_open(j, _):
        rs_put(RIGHT, K, j, False)
        rs_put(LEFT, K, 2 + j, False)
        return 0

    def rs_open2(j, _):
        rs_put(RIGHT, K - 1, 2 + j, False)
        rs_put(LEFT, K - 1, j, False)
        return 0

    lax.fori_loop(0, 2, rs_open, 0)
    lax.fori_loop(0, 2, rs_open2, 0)
    lax.fori_loop(3, Z, middle, 0)

    acc = jnp.zeros((32, QC), F32)
    fit = jnp.zeros((1, ROWS), F32)
    for p in range(Q):
        acc = acc + nt(gr[p], h2[:, p * ROWS : (p + 1) * ROWS])
        x = gr[p].astype(F32)
        fit = fit + x[ACT : ACT + 1, :] + x[ACT + 1 : ACT + 2, :]
    at_head = lax.broadcasted_iota(jnp.int32, (24, QC), 0)
    dH[z] = jnp.where(at_head == ACT, fit, acc[0:24, :])

    def dh_copy(way, k):
        b = at(1 - k) if way == RIGHT else at(k - 1)
        return copy(dH.at[b], dH.at[b], dh_s.at[way, k - 1], dh_r.at[way, k - 1], side[way])

    def dh_in(way, k):
        b = at(-k) if way == RIGHT else at(k)
        copy(dH.at[b], dH.at[b], dh_s.at[way, k - 1], dh_r.at[way, k - 1], side[way]).wait_recv()

    dh_copy(RIGHT, 1).start()
    dh_copy(LEFT, 1).start()

    def rs_join(j, _):
        rs_put(RIGHT, K - 1, j, True)
        rs_put(LEFT, K - 1, 2 + j, True)
        return 0

    lax.fori_loop(0, 2, rs_join, 0)

    def back(i, _):
        k = 2 - i // 4
        p = lax.rem(i, 4)

        feats = pl.ds(pl.multiple_of(i * 256, 256), 256)
        w = wq[i].reshape(BK, QC)

        def tile(r, acc):
            rows = pl.ds(pl.multiple_of(r * ROWS, ROWS), ROWS)
            g = (nn(w, g2[:, rows]) * s1[feats, rows].astype(F32)).astype(BF16)
            return acc + nt(obT[:, rows], g)

        dI[:, :, :, :, feats] = lax.fori_loop(0, Q, tile, jnp.zeros((OBS, 256), F32)).reshape(Z, 2, 2, 8, 256)
        rs_put(RIGHT, k, p, True)
        rs_put(LEFT, k, p, True)

        @pl.when(i == 2)
        def _():
            dh_in(RIGHT, 1)
            dh_in(LEFT, 1)
            dh_copy(RIGHT, 2).start()
            dh_copy(LEFT, 2).start()

        @pl.when(i == 4)
        def _():
            dh_in(RIGHT, 2)
            dh_in(LEFT, 2)
            dh_copy(RIGHT, 3).start()
            dh_copy(LEFT, 3).start()

        @pl.when(i == 6)
        def _():
            dh_in(RIGHT, 3)
            dh_in(LEFT, 3)
            dh_copy(RIGHT, 4).start()

        return 0

    lax.fori_loop(0, Z, back, 0)

    for b in range(Z):
        for j in range(2):
            sib_s[b, j] = dI[b, j, 1 - c].astype(BF16)
    core_sum = copy(sib_s, sib_r, sb_s.at[2], sb_r.at[2], sib)
    core_sum.start()
    core_sum.wait_recv()

    def own_in(off, j):
        b = at(off)
        return dI[b, j, c] + sib_r[b, j].astype(F32)

    def ri_copy(way, k, j):
        return copy(
            ris.at[way, k - 1, j], rib.at[way, k - 1, j], ri_s.at[way, k - 1, j], ri_r.at[way, k - 1, j], side[way]
        )

    def ri_in(way, k, j):
        copy(rib.at[way, k, j], rib.at[way, k, j], ri_s.at[way, k, j], ri_r.at[way, k, j], side[way]).wait_recv()
        return rib[way, k, j].astype(F32)

    def ri_put(way, k, j, joined):
        v = own_in(k if way == RIGHT else -k, j)
        if joined:
            v = v + ri_in(way, k, j)
        ris[way, k - 1, j] = v.astype(BF16)
        ri_copy(way, k, j).start()

    ri_put(RIGHT, 4, 0, False)
    ri_put(LEFT, 4, 1, False)
    ri_put(RIGHT, 3, 1, False)
    ri_put(LEFT, 3, 0, False)

    lr = lrate[m]
    rate = jnp.exp(jnp.full((8, 128), lr, F32))[0:1, 0:1]
    flag = copyf[m]

    def middle_end(t):
        p = mate(t)
        g = dW[z, p] + rs_in(RIGHT, 0, p) + rs_in(LEFT, 0, p)
        nm[p] = (wq[z, p].astype(F32) - rate * g).astype(BF16)
        copy(nm.at[p], ym.at[p], y_s.at[p], y_r.at[p], after).start()

    middle_end(2)
    ri_put(RIGHT, 3, 0, True)
    ri_put(LEFT, 3, 1, True)
    middle_end(1)
    dh_in(RIGHT, 4)
    tot = dH[0]
    for b in range(1, Z):
        tot = tot + dH[b]
    dHg[q] = tot
    o_fit[0] = jnp.sum(tot[ACT : ACT + 1, :])

    def dh_mate(t):
        return copy(dHg.at[q], dHg.at[q], gp_s.at[DH, mate(t)], gp_r.at[DH, q], mate_id(t))

    for t in (2, 1, 3):
        dh_mate(t).start()
    for j in range(2):
        ri_put(RIGHT, 2, j, True)
        ri_put(LEFT, 2, j, True)
    middle_end(3)
    middle_end(0)
    for j in range(2):
        ri_put(RIGHT, 1, j, True)
        ri_put(LEFT, 1, j, True)

    def chosen(got, own):
        return jnp.where(jnp.full(own.shape, flag) == 1, got.astype(F32), own.astype(F32)).astype(BF16)

    def out_mate(p):
        return copy(nm.at[p], om.at[q], gp_s.at[OUT, p], gp_r.at[OUT, q], {"dp": z * Q + p})

    def middle_pick(t):
        p = mate(t)
        copy(nm.at[p], ym.at[p], y_s.at[p], y_r.at[p], after).wait()
        nm[p] = chosen(ym[p], nm[p])
        if t:
            out_mate(p).start()
        else:
            om[q] = nm[p]

    middle_pick(2)
    middle_pick(1)

    for t in (2, 1, 3):
        p = mate(t)
        copy(dHg.at[p], dHg.at[p], gp_s.at[DH, p], gp_r.at[DH, p], sib).wait_recv()
    tH[...] = jnp.transpose(dHg[z // 2])
    own_rows = pl.ds(pl.multiple_of(lax.rem(d, Z) * 64, 64), 64)
    nh[...] = (wh[z, h, c].astype(F32) - rate * tH[own_rows, 0:ACT]).astype(BF16)
    head_y = copy(nh, yh, y_s.at[5], y_r.at[5], after)
    head_y.start()
    middle_pick(3)
    middle_pick(0)
    for j in range(2):
        tin[j] = own_in(0, j) + ri_in(RIGHT, 0, j) + ri_in(LEFT, 0, j)
    xs[...] = tin[1 - h].astype(BF16)
    cross = copy(xs, xr, xp_s.at[2], xp_r.at[2], xpt)
    cross.start()
    head_y.wait_recv()
    o_head[...] = chosen(yh[...], nh[...])
    cross.wait_recv()
    ni[...] = (wi[z, h, c].astype(F32) - rate * (tin[h] + xr[...].astype(F32))).astype(BF16)
    in_y = copy(ni, yi, y_s.at[4], y_r.at[4], after)
    in_y.start()
    for t in (2, 1, 3):
        p = mate(t)
        copy(om.at[p], om.at[p], gp_s.at[OUT, p], gp_r.at[OUT, p], sib).wait_recv()
    for p in range(Q):
        o_mid[:, p * QC : (p + 1) * QC] = om[p]
    lr_before = lrate[lax.rem(m + POP - 1, POP)]
    pick = pert[m]
    o_rate[0] = jnp.where(flag == 1, lr_before, lr) + jnp.where(pick == 0, -0.2, jnp.where(pick == 1, 0.0, 0.2))
    in_y.wait_recv()
    o_in[...] = chosen(yi[...], ni[...])

    xwi.wait_send()
    xwh.wait_send()
    cross.wait_send()
    head_y.wait_send()
    in_y.wait_send()
    core_copy(wi, 0).wait_send()
    core_copy(wh, 1).wait_send()
    core_sum.wait_send()
    for t in (1, 2, 3):
        quarter(t).wait_send()
        sight(t).wait_send()
        raw_out(mate(t)).wait_send()
        gr_out(t).wait_send()
        dh_mate(t).wait_send()
        out_mate(mate(t)).wait_send()
    for k in range(1, K):
        for way in (RIGHT, LEFT):
            for j in range(2):
                for kind in (WI, WM, WH):
                    ag(kind, way, k, j).wait_send()
                ri_copy(way, k, j).wait_send()
            for p in range(Q):
                rs_copy(way, k, p).wait_send()
            dh_copy(way, k).wait_send()
    for kind in (WI, WM, WH):
        ag(kind, RIGHT, K, 0).wait_send()
        ag(kind, LEFT, K, 1).wait_send()
    ri_copy(RIGHT, K, 0).wait_send()
    ri_copy(LEFT, K, 1).wait_send()
    for j in range(2):
        rs_copy(RIGHT, K, j).wait_send()
        rs_copy(LEFT, K, 2 + j).wait_send()
    dh_copy(RIGHT, K).wait_send()


def local(observations, returns, actions, w_input, w_middle, w_head, log_rate, copy_from, perturb):
    hbm = pl.BlockSpec(memory_space=pltpu.HBM)
    vmem = pl.BlockSpec(memory_space=pltpu.VMEM)
    smem = pl.BlockSpec(memory_space=pltpu.SMEM)
    V = pltpu.VMEM
    S = pltpu.SemaphoreType.DMA
    out = pl.pallas_call(
        kernel,
        out_shape=(
            jax.ShapeDtypeStruct((8, D), BF16),
            jax.ShapeDtypeStruct((64, D), BF16),
            jax.ShapeDtypeStruct((64, ACT), BF16),
            jax.ShapeDtypeStruct((1,), F32),
            jax.ShapeDtypeStruct((1,), F32),
        ),
        in_specs=[hbm, vmem, vmem, hbm, hbm, hbm, smem, smem, smem],
        out_specs=(vmem, vmem, vmem, smem, smem),
        scratch_shapes=[
            V((Q, ROWS, OBS), BF16),
            V((OBS, D), BF16),
            V((Z, 2, 2, 8, D), BF16),
            V((Z, 2, 2, 64, ACT), BF16),
            V((Z, Q, 64, QC), BF16),
            V((D, OBS), BF16),
            V((QC, BK), BF16),
            V((D, D), BF16),
            V((D, D), BF16),
            V((QC, D), F32),
            V((QC, D), BF16),
            V((QC, D), BF16),
            V((QC, 128), F32),
            V((32, QC), BF16),
            V((Q, 24, ROWS), F32),
            V((Q, 24, ROWS), F32),
            V((Q, 32, ROWS), BF16),
            V((Z, Q, 64, QC), F32),
            V((2, K, Q, 64, QC), BF16),
            V((2, K, Q, 64, QC), BF16),
            V((Z, 2, 2, 8, D), F32),
            V((Z, 2, 8, D), BF16),
            V((Z, 2, 8, D), BF16),
            V((2, K, 2, 8, D), BF16),
            V((2, K, 2, 8, D), BF16),
            V((2, 8, D), F32),
            V((8, D), BF16),
            V((8, D), BF16),
            V((Z, 24, QC), F32),
            V((Q, 24, QC), F32),
            V((QC, 24), F32),
            V((Q, 64, QC), BF16),
            V((Q, 64, QC), BF16),
            V((Q, 64, QC), BF16),
            V((8, D), BF16),
            V((8, D), BF16),
            V((64, ACT), BF16),
            V((64, ACT), BF16),
            S((3, 2, K, 2)), S((3, 2, K, 2)),
            S((6, Q)), S((6, Q)),
            S((3,)), S((3,)),
            S((3,)), S((3,)),
            S((2, K)), S((2, K)),
            S((2, K, Q)), S((2, K, Q)),
            S((2, K, 2)), S((2, K, 2)),
            S((6,)), S((6,)),
            S((4,)),
        ],
        compiler_params=pltpu.CompilerParams(
            collective_id=0, has_side_effects=True, vmem_limit_bytes=64 * 1024 * 1024 - 65536
        ),
    )(observations[0], returns, actions, w_input[0], w_middle[0], w_head[0], log_rate, copy_from, perturb)
    return out[0][None], out[1][None], out[2][None], out[3], out[4]


def solution(mesh):
    in_specs = (
        P("pop", "dp", None),
        P("pop", "dp"),
        P("pop", "dp"),
        P("pop", "dp", None),
        P("pop", "dp", None),
        P("pop", "dp", None),
        P(),
        P(),
        P(),
    )
    out_specs = (
        P("pop", "dp", None),
        P("pop", "dp", None),
        P("pop", "dp", None),
        P("pop"),
        P("pop"),
    )
    return jax.shard_map(local, mesh=mesh, in_specs=in_specs, out_specs=out_specs, check_vma=False)
```

```python
import jax
import jax.numpy as jnp
from jax import lax
from jax.experimental import pallas as pl
from jax.experimental.pallas import tpu as pltpu
from jax.sharding import PartitionSpec as P

F32 = jnp.float32
BF16 = jnp.bfloat16
Z = 8
K = Z // 2
Q = 4
ROWS = 512
OBS = 256
D = 2048
QC = D // Q
BK = D // Z
ACT = 18
POP = 8
BATCH = ROWS * Z * Q
WM, WH = 0, 1
OB, QT, RAW, GR, DH, OUT = range(6)
RIGHT, LEFT = 0, 1
NEAR = (1, -1, 2, -2, 3, -3, K)


def nt(a, b):
    return lax.dot_general(a, b, (((1,), (1,)), ((), ())), preferred_element_type=F32)


def nn(a, b):
    return jnp.dot(a, b, preferred_element_type=F32)


def kernel(
    obs, ret, act, win, wmid, whead, lrate, copyf, pert,
    o_in, o_mid, o_head, o_rate, o_fit,
    ob, obT, wi, wh, wq, w1T, wT, dT, h1, s1, p2, h2, g2, whp, whq, whT,
    raw_s, raw_r, gr, dW, rss, rsb, dI, sib_s, sib_r, ris, rib, tin, xs, xr,
    xp, wp, dH, dHg, tH, nm, ym, om, ni, yi, nh, yh,
    ag_s, ag_r, wz_s, wz_r, wx_s, wx_r, gp_s, gp_r, xp_s, xp_r, sb_s, sb_r, dh_s, dh_r, rs_s, rs_r, ri_s, ri_r, y_s, y_r, loc,
):
    m = lax.axis_index("pop")
    d = lax.axis_index("dp")
    z = d // Q
    q = lax.rem(d, Q)
    h = q // 2
    c = lax.rem(q, 2)
    sib = {"dp": z * Q + h * 2 + (1 - c)}
    xpt = {"dp": z * Q + (1 - h) * 2 + c}
    side = [{"dp": lax.rem(z + 1, Z) * Q + q}, {"dp": lax.rem(z + Z - 1, Z) * Q + q}]
    after = {"pop": lax.rem(m + 1, POP)}
    m_after = lax.rem(m + 1, POP)
    m_before = lax.rem(m + POP - 1, POP)
    before = {"pop": m_before}

    def mate(t):
        return lax.rem(q + t, Q)

    def mate_id(t):
        return {"dp": z * Q + mate(t)}

    def at(off):
        return lax.rem(z + off + Z, Z)

    def column(off):
        return {"dp": at(off) * Q + q}

    def copy(src, dst, ss, rs, dev):
        return pltpu.make_async_remote_copy(
            src_ref=src, dst_ref=dst, send_sem=ss, recv_sem=rs, device_id=dev,
            device_id_type=pl.DeviceIdType.MESH,
        )

    fetch = [
        pltpu.make_async_copy(win, wi.at[z, h, c], loc.at[0]),
        pltpu.make_async_copy(wmid.at[:, pl.ds(pl.multiple_of(q * QC, QC), QC)], wq.at[z, q], loc.at[1]),
        pltpu.make_async_copy(whead, wh.at[z, h, c], loc.at[2]),
        pltpu.make_async_copy(obs, ob.at[q], loc.at[3]),
    ]
    for f in fetch:
        f.start()

    barrier = pltpu.get_barrier_semaphore()
    met = [mate_id(t) for t in (1, 2, 3)] + [after, before] + [column(off) for off in (2, -2, 1, -1)]
    for near in (m_after, m_before):
        met += [{"pop": near, "dp": z * Q + mate(t)} for t in (1, 2, 3)]
    for dev in met:
        pl.semaphore_signal(barrier, inc=1, device_id=dev, device_id_type=pl.DeviceIdType.MESH)
    pl.semaphore_wait(barrier, len(met))

    def win_out(off):
        i = NEAR.index(off)
        return copy(win, wi.at[z, h, c], wz_s.at[i], wz_r.at[i], column(off))

    def win_in(off):
        i = NEAR.index(off)
        ref = wi.at[at(-off), h, c]
        copy(ref, ref, wz_s.at[i], wz_r.at[i], xpt).wait_recv()

    def win_x(off):
        i = 7 if off == 0 else NEAR.index(off)
        ref = wi.at[at(-off), h, c]
        return copy(win if off == 0 else ref, ref, wx_s.at[i], wx_r.at[i], xpt)

    def win_x_in(off):
        i = 7 if off == 0 else NEAR.index(off)
        ref = wi.at[at(-off), 1 - h, c]
        copy(ref, ref, wx_s.at[i], wx_r.at[i], xpt).wait_recv()

    def win_on(step, off):
        i = NEAR.index(off)
        ref = wi.at[at(-2 * step), h, c]
        return copy(ref, ref, wz_s.at[i], wz_r.at[i], column(off - 2 * step))

    for off in (2, -2, 1, -1):
        win_out(off).start()
    win_x(0).start()
    prior = copy(win, wp, y_s.at[6], y_r.at[6], after)
    xwh = copy(whead, wh.at[z, h, c], xp_s.at[1], xp_r.at[1], xpt)

    def quarter(t):
        p = mate(t)
        return copy(
            wmid.at[:, pl.ds(pl.multiple_of(p * QC, QC), QC)], wq.at[z, q], gp_s.at[QT, p], gp_r.at[QT, q], mate_id(t)
        )

    x_mate = (1 - h) * 2 + c
    sight_x = copy(obs, ob.at[q], gp_s.at[OB, 0], gp_r.at[OB, q], xpt)
    sight_core = copy(obs, ob.at[q], gp_s.at[OB, 1], gp_r.at[OB, q], sib)
    sight_on = copy(ob.at[x_mate], ob.at[x_mate], gp_s.at[OB, 2], gp_r.at[OB, x_mate], sib)

    def quarter_in(p):
        copy(wq.at[z, p], wq.at[z, p], gp_s.at[QT, p], gp_r.at[QT, p], sib).wait_recv()

    for t in (1, 2, 3):
        quarter(t).start()
    xwh.start()
    sight_core.start()
    prior.start()
    p2[...] = jnp.zeros_like(p2)
    dT[...] = jnp.zeros_like(dT)

    def piece(kind, b, j):
        if kind == WM:
            return wq.at[b, pl.ds(2 * j, 2)]
        return wh.at[b, j, c]

    def ag(kind, way, k, j):
        b = at(1 - k) if way == RIGHT else at(k - 1)
        ref = piece(kind, b, j)
        return copy(ref, ref, ag_s.at[kind, way, k - 1, j], ag_r.at[kind, way, k - 1, j], side[way])

    def ag_in(kind, way, k, j):
        b = at(-k) if way == RIGHT else at(k)
        ref = piece(kind, b, j)
        copy(ref, ref, ag_s.at[kind, way, k - 1, j], ag_r.at[kind, way, k - 1, j], side[way]).wait_recv()

    def put(kinds, k, j):
        for kind in kinds:
            for way in (RIGHT, LEFT):
                ag(kind, way, k, j).start()

    def take(kinds, k, j):
        for kind in kinds:
            for way in (RIGHT, LEFT):
                ag_in(kind, way, k, j)

    def take_last(kinds, k):
        for kind in kinds:
            ag_in(kind, RIGHT, k, 0)
            ag_in(kind, LEFT, k, 1)

    def put_last(kinds):
        for kind in kinds:
            ag(kind, RIGHT, K, 0).start()
            ag(kind, LEFT, K, 1).start()

    MID = (WM, WH)

    def core_copy(off, i):
        b = at(-off)
        return copy(wi.at[b, :, c], wi.at[b, :, c], sb_s.at[i], sb_r.at[i], sib)

    def core_in(off, i):
        b = at(-off)
        copy(wi.at[b, :, 1 - c], wi.at[b, :, 1 - c], sb_s.at[i], sb_r.at[i], sib).wait_recv()

    core_off = (0,) + NEAR
    head_core = copy(wh.at[:, :, c], wh.at[:, :, c], sb_s.at[9], sb_r.at[9], sib)

    def head_core_in():
        copy(wh.at[:, :, 1 - c], wh.at[:, :, 1 - c], sb_s.at[9], sb_r.at[9], sib).wait_recv()

    for off in NEAR[:2]:
        win_in(off)
        win_x(off).start()
    fetch[1].wait()
    fetch[2].wait()
    quarter_in(h * 2 + (1 - c))
    put(MID, 1, h)
    for off in NEAR[2:4]:
        win_in(off)
        win_on(off // 2, 3 * off // 2).start()
        if off > 0:
            win_on(1, K).start()
        win_x(off).start()
    for off in NEAR[4:]:
        win_in(off)
        win_x(off).start()
    sight_x.start()
    fetch[0].wait()
    quarter_in((1 - h) * 2)
    quarter_in((1 - h) * 2 + 1)
    xwh.wait_recv()
    put(MID, 1, 1 - h)
    for i, off in enumerate(core_off[:3]):
        win_x_in(off)
        core_copy(off, i).start()
    take(MID, 1, h)
    put(MID, 2, h)
    for i, off in enumerate(core_off[3:]):
        win_x_in(off)
        core_copy(off, 3 + i).start()
    def obs_in(p):
        copy(ob.at[p], ob.at[p], gp_s.at[OB, 0], gp_r.at[OB, p], sib).wait_recv()

    fetch[3].wait()
    obs_in(h * 2 + (1 - c))

    def turn(p):
        cols = pl.ds(pl.multiple_of(p * ROWS, ROWS), ROWS)
        obT[:, cols] = jnp.transpose(ob[p].astype(F32)).astype(BF16)

    def group_at(i):
        return (h + i // 2 * (1 - 2 * h)) * 2 + c + i % 2 * (1 - 2 * c)

    def turn_by(i, _):
        turn(group_at(i))
        return 0

    lax.fori_loop(0, 2, turn_by, 0)
    take(MID, 1, 1 - h)
    put(MID, 2, 1 - h)
    for i in range(8):
        core_in(core_off[i], i)

    def turn_in(i, _):
        cols = pl.ds(pl.multiple_of(i * 256, 256), 256)
        x = wi[:, :, :, :, cols].astype(F32).reshape(OBS, 256)
        w1T[cols, :] = (0.5 * jnp.transpose(x)).astype(BF16)
        return 0

    lax.fori_loop(0, D // 256, turn_in, 0)

    def block_of(i):
        return at(((i + 1) // 2) * (2 * lax.rem(i + 1, 2) - 1))

    def first(i, p):
        feats = pl.ds(pl.multiple_of(block_of(i) * BK, BK), BK)
        rows = slice(p * ROWS, (p + 1) * ROWS)
        u = nn(w1T[feats, :], obT[:, rows])
        t = jnp.tanh(u)
        a = 1.0 + t
        hid = u * a
        h1[feats, rows] = hid.astype(BF16)
        s1[feats, rows] = (a + hid * (1.0 - t)).astype(BF16)

    def turn_w(i):
        wT[...] = (0.5 * jnp.transpose(wq[block_of(i)].astype(F32).reshape(BK, QC))).astype(BF16)

    def second(i, p):
        feats = pl.ds(pl.multiple_of(block_of(i) * BK, BK), BK)
        rows = slice(p * ROWS, (p + 1) * ROWS)
        p2[:, rows] += nn(wT[...], h1[feats, rows])

    def first_by(i, _):
        @pl.when(i == 0)
        def _():
            with jax.named_scope("wait0"):
                take(MID, 2, h)
                put(MID, 3, h)

        @pl.when(i == 2)
        def _():
            with jax.named_scope("wait2"):
                take(MID, 2, 1 - h)
                put(MID, 3, 1 - h)

        @pl.when(i == 6)
        def _():
            with jax.named_scope("wait6"):
                take_last(MID, 3)
                put_last(MID)

        for p in range(Q):
            first(i, p)
        return 0

    def second_by(i, _):
        @pl.when(i == 5)
        def _():
            with jax.named_scope("wait5s"):
                for kind in MID:
                    ag_in(kind, RIGHT, 3, 1)
                    ag_in(kind, LEFT, 3, 0)

        turn_w(i)
        for p in range(Q):
            second(i, p)
        return 0

    obs_in(x_mate)
    sight_on.start()
    turn_by(2, 0)
    obs_in((1 - h) * 2 + (1 - c))
    turn_by(3, 0)
    lax.fori_loop(0, Z, first_by, 0)
    lax.fori_loop(0, Z - 1, second_by, 0)
    take_last(MID, K)
    head_core.start()
    turn_w(Z - 1)
    for p in range(Q):
        second(Z - 1, p)

    head_core_in()
    whp[...] = jnp.zeros_like(whp)
    for b in range(2):
        for i in range(Q):
            lanes = slice((b * Q + i) * 64, (b * Q + i + 1) * 64)
            whp[0:ACT, lanes] = wh[2 * q + b, i // 2, i % 2].astype(F32)
    whT[...] = whp[0:32, :].astype(BF16)
    whq[...] = jnp.transpose(whp[...]).astype(BF16)

    def raw_out(p):
        return copy(raw_s.at[p], raw_r.at[q], gp_s.at[RAW, p], gp_r.at[RAW, q], {"dp": z * Q + p})

    for t in (2, 1, 3, 0):
        p = mate(t)
        rows = pl.ds(pl.multiple_of(p * ROWS, ROWS), ROWS)

        def forward2(i, _):
            cols = pl.ds(pl.multiple_of(p * ROWS + i * 128, 128), 128)
            u = p2[:, cols]
            h2[:, cols] = (u + u * jnp.tanh(u)).astype(BF16)
            return 0

        lax.fori_loop(0, 4, forward2, 0)
        raw_s[p] = nn(whT[...], h2[:, rows])[0:24, :]
        if t:
            raw_out(p).start()
    def slope2(i, _):
        cols = pl.ds(pl.multiple_of(i * 128, 128), 128)
        u = p2[:, cols]
        t = jnp.tanh(u)
        a = 1.0 + t
        p2[:, cols] = a + u * a * (1.0 - t)
        return 0

    lax.fori_loop(0, D // 128, slope2, 0)
    raw = raw_s[q]
    for t in (2, 1, 3):
        p = mate(t)
        copy(raw_r.at[p], raw_r.at[p], gp_s.at[RAW, p], gp_r.at[RAW, p], sib).wait_recv()
        raw = raw + raw_r[p]
    at_act = lax.broadcasted_iota(jnp.int32, raw.shape, 0)
    squash = jnp.tanh(raw * 0.5)
    logits = 2.0 * squash
    e = jnp.where(at_act < ACT, jnp.exp(logits), 0.0)
    total = jnp.sum(e, axis=0, keepdims=True)
    logp = logits - jnp.log(total)
    onehot = jnp.where(at_act == act[...], 1.0, 0.0)
    gains = ret[...] * (1.0 / BATCH)
    term = gains * jnp.sum(logp * onehot, axis=0, keepdims=True)
    grad = -gains * (onehot - e / total) * (1.0 - squash * squash)
    high = term.astype(BF16).astype(F32)
    low = term - high
    grad = jnp.where(at_act < ACT, grad, jnp.where(at_act == ACT, high, jnp.where(at_act == ACT + 1, low, 0.0)))
    gr[q] = jnp.concatenate([grad, jnp.zeros((8, ROWS), F32)], axis=0).astype(BF16)

    def gr_out(t):
        return copy(gr.at[q], gr.at[q], gp_s.at[GR, mate(t)], gp_r.at[GR, q], mate_id(t))

    for t in (2, 1, 3):
        gr_out(t).start()
    wb = (0.5 * whq[:, 0:32].astype(F32)).astype(BF16)

    def grad2(i):
        p = group_at(i)
        if i:
            copy(gr.at[p], gr.at[p], gp_s.at[GR, p], gp_r.at[GR, p], sib).wait_recv()
        rows = pl.ds(pl.multiple_of(p * ROWS, ROWS), ROWS)
        g2[:, rows] = (nn(wb, gr[p]) * p2[:, rows]).astype(BF16)

    def back(i, _):
        p = group_at(i // 2)
        rows = pl.ds(pl.multiple_of(p * ROWS, ROWS), ROWS)
        half = lax.rem(i, 2)
        feats = pl.ds(pl.multiple_of(half * (D // 2), D // 2), D // 2)
        w = wq[pl.ds(half * (Z // 2), Z // 2)].reshape(D // 2, QC)
        g = (nn(w, g2[:, rows]) * s1[feats, rows].astype(F32)).astype(BF16)
        dT[feats, :] += nn(g, ob[p])
        return 0

    grad2(0)
    lax.fori_loop(0, 2, back, 0)
    grad2(1)
    grad2(2)
    grad2(3)

    def middle(i, _):
        one = at(K + i)
        two = at(K - 1 - i)
        at_one = pl.ds(pl.multiple_of(one * BK, BK), BK)
        at_two = pl.ds(pl.multiple_of(two * BK, BK), BK)
        both = nt(jnp.concatenate([h1[at_one, :], h1[at_two, :]], axis=0), g2[...])
        dW[one] = both[0:BK].reshape(Q, BK // Q, QC)
        dW[two] = both[BK:].reshape(Q, BK // Q, QC)
        return 0

    def rs_copy(way, k, p):
        return copy(
            rss.at[way, k - 1, p], rsb.at[way, k - 1, p], rs_s.at[way, k - 1, p], rs_r.at[way, k - 1, p], side[way]
        )

    def rs_in(way, k, p):
        copy(rsb.at[way, k, p], rsb.at[way, k, p], rs_s.at[way, k, p], rs_r.at[way, k, p], side[way]).wait_recv()
        return rsb[way, k, p].astype(F32)

    def rs_put(way, k, p, joined):
        v = dW[at(k if way == RIGHT else -k), p]
        if joined:
            v = v + rs_in(way, k, p)
        rss[way, k - 1, p] = v.astype(BF16)
        rs_copy(way, k, p).start()

    def rs_open(j, _):
        rs_put(RIGHT, K, j, False)
        rs_put(LEFT, K, 2 + j, False)
        return 0

    def rs_open2(j, _):
        rs_put(RIGHT, K - 1, 2 + j, False)
        rs_put(LEFT, K - 1, j, False)
        return 0

    def middle_open(i, _):
        middle(i, 0)

        @pl.when(i == 0)
        def _():
            lax.fori_loop(0, 2, rs_open, 0)

        return 0

    lax.fori_loop(0, 2, middle_open, 0)
    lax.fori_loop(0, 2, rs_open2, 0)

    acc = jnp.zeros((32, QC), F32)
    fit = jnp.zeros((1, ROWS), F32)
    for p in range(Q):
        acc = acc + nt(gr[p], h2[:, p * ROWS : (p + 1) * ROWS])
        x = gr[p].astype(F32)
        fit = fit + x[ACT : ACT + 1, :] + x[ACT + 1 : ACT + 2, :]
    at_head = lax.broadcasted_iota(jnp.int32, (24, QC), 0)
    fit_high = fit.astype(BF16).astype(F32)
    packed = jnp.where(at_head == ACT, fit_high, jnp.where(at_head == ACT + 1, fit - fit_high, acc[0:24, :]))
    dH[z] = packed.astype(BF16)

    def dh_out(off):
        i = NEAR.index(off)
        return copy(dH.at[z], dH.at[z], dh_s.at[i], dh_r.at[i], column(off))

    def dh_on(step, off):
        i = NEAR.index(off)
        ref = dH.at[at(-2 * step)]
        return copy(ref, ref, dh_s.at[i], dh_r.at[i], column(off - 2 * step))

    def dh_in(off):
        i = NEAR.index(off)
        ref = dH.at[at(-off)]
        copy(ref, ref, dh_s.at[i], dh_r.at[i], sib).wait_recv()

    for off in (2, -2, 1, -1):
        dh_out(off).start()

    def join3(j, _):
        rs_put(RIGHT, K - 1, j, True)
        rs_put(LEFT, K - 1, 2 + j, True)
        return 0

    def join2(j, _):
        rs_put(RIGHT, 2, lax.rem(2 + j, Q), True)
        rs_put(LEFT, 2, j, True)
        return 0

    lax.fori_loop(2, 4, back, 0)
    lax.fori_loop(0, 2, join3, 0)
    lax.fori_loop(4, 8, back, 0)

    def turn_back(i, _):
        feats = pl.ds(pl.multiple_of(i * 256, 256), 256)
        x = 0.5 * jnp.transpose(dT[feats, :])
        dI[:, :, :, :, feats] = x.reshape(Z, 2, 2, 8, 256)
        return 0

    dh_in(2)
    dh_on(1, 3).start()
    dh_on(1, K).start()
    dh_in(-2)
    dh_on(-1, -3).start()
    lax.fori_loop(0, Z, turn_back, 0)

    for b in range(Z):
        for j in range(2):
            sib_s[b, j] = dI[b, j, 1 - c].astype(BF16)
    core_sum = copy(sib_s, sib_r, sb_s.at[8], sb_r.at[8], sib)
    core_sum.start()
    lax.fori_loop(2, 4, middle, 0)
    core_sum.wait_recv()

    def own_in(off, j):
        b = at(off)
        return dI[b, j, c] + sib_r[b, j].astype(F32)

    def ri_copy(way, k, j):
        return copy(
            ris.at[way, k - 1, j], rib.at[way, k - 1, j], ri_s.at[way, k - 1, j], ri_r.at[way, k - 1, j], side[way]
        )

    def ri_in(way, k, j):
        copy(rib.at[way, k, j], rib.at[way, k, j], ri_s.at[way, k, j], ri_r.at[way, k, j], side[way]).wait_recv()
        return rib[way, k, j].astype(F32)

    def ri_put(way, k, j, joined):
        v = own_in(k if way == RIGHT else -k, j)
        if joined:
            v = v + ri_in(way, k, j)
        ris[way, k - 1, j] = v.astype(BF16)
        ri_copy(way, k, j).start()

    ri_put(RIGHT, 4, 0, False)
    ri_put(LEFT, 4, 1, False)
    ri_put(RIGHT, 3, 1, False)
    ri_put(LEFT, 3, 0, False)

    lr = lrate[m]
    lr_before = lrate[m_before]
    rate = jnp.exp(jnp.full((8, 128), lr, F32))[0:1, 0:1]
    rate_before = jnp.exp(jnp.full((8, 128), lr_before, F32))[0:1, 0:1]
    flag = copyf[m]

    def next_out(p):
        return copy(nm.at[p], ym.at[q], y_s.at[p], y_r.at[q], {"pop": m_after, "dp": z * Q + p})

    def out_mate(p):
        return copy(nm.at[p], om.at[q], gp_s.at[OUT, p], gp_r.at[OUT, q], {"dp": z * Q + p})

    def middle_end(p):
        g = dW[z, p] + rs_in(RIGHT, 0, p) + rs_in(LEFT, 0, p)
        nm[p] = (wq[z, p].astype(F32) - rate * g).astype(BF16)
        next_out(p).start()

        @pl.when(p != q)
        def _():
            out_mate(p).start()

    def ones(j, _):
        rs_put(RIGHT, 1, lax.rem(2 + j, Q), True)
        rs_put(LEFT, 1, j, True)
        return 0

    lax.fori_loop(0, 2, join2, 0)
    ri_put(RIGHT, 3, 0, True)
    ri_put(LEFT, 3, 1, True)
    lax.fori_loop(2, 4, join2, 0)
    for off in (1, -1, 3, -3, K):
        dh_in(off)
    tot = dH[0].astype(F32)
    for b in range(1, Z):
        tot = tot + dH[b].astype(F32)
    dHg[q] = tot
    o_fit[0] = jnp.sum(tot[ACT : ACT + 2, :])

    def dh_mate(t):
        return copy(dHg.at[q], dHg.at[q], gp_s.at[DH, mate(t)], gp_r.at[DH, q], mate_id(t))

    for t in (2, 1, 3):
        dh_mate(t).start()

    lax.fori_loop(0, 2, ones, 0)
    for j in range(2):
        ri_put(RIGHT, 2, j, True)
        ri_put(LEFT, 2, j, True)
    lax.fori_loop(2, 4, ones, 0)
    for t in (2, 1, 3):
        p = mate(t)
        copy(dHg.at[p], dHg.at[p], gp_s.at[DH, p], gp_r.at[DH, p], sib).wait_recv()
    tH[...] = jnp.transpose(dHg[z // 2])
    own_rows = pl.ds(pl.multiple_of(lax.rem(d, Z) * 64, 64), 64)
    nh[...] = (wh[z, h, c].astype(F32) - rate * jnp.transpose(tH[own_rows, :])[0:ACT, :]).astype(BF16)
    head_y = copy(nh, yh, y_s.at[5], y_r.at[5], after)
    head_y.start()
    middle_end(0)
    middle_end(2)
    for j in range(2):
        ri_put(RIGHT, 1, j, True)
        ri_put(LEFT, 1, j, True)
    middle_end(1)
    middle_end(3)
    def chosen(got, own):
        return jnp.where(jnp.full(own.shape, flag) == 1, got.astype(F32), own.astype(F32)).astype(BF16)

    for j in range(2):
        tin[j] = own_in(0, j) + ri_in(RIGHT, 0, j) + ri_in(LEFT, 0, j)
    xs[...] = tin[1 - h].astype(BF16)
    cross = copy(xs, xr, xp_s.at[2], xp_r.at[2], xpt)
    cross.start()
    cross_y = copy(xs, xp, xp_s.at[0], xp_r.at[0], {"pop": m_after, "dp": xpt["dp"]})
    cross_y.start()
    ni[...] = tin[h].astype(BF16)
    in_y = copy(ni, yi, y_s.at[4], y_r.at[4], after)
    in_y.start()
    head_y.wait_recv()
    o_head[...] = chosen(yh[...], nh[...])
    for t in (0, 1, 2, 3):
        p = mate(t)
        own = nm.at[p] if t == 0 else om.at[p]
        if t:
            copy(own, own, gp_s.at[OUT, p], gp_r.at[OUT, p], sib).wait_recv()
        copy(ym.at[p], ym.at[p], y_s.at[p], y_r.at[p], after).wait_recv()
        o_mid[:, pl.ds(pl.multiple_of(p * QC, QC), QC)] = chosen(ym[p], own[...])
    pick = pert[m]
    o_rate[0] = jnp.where(flag == 1, lr_before, lr) + jnp.where(pick == 0, -0.2, jnp.where(pick == 1, 0.0, 0.2))
    prior.wait_recv()
    cross.wait_recv()
    cross_y.wait_recv()
    in_y.wait_recv()
    new = wi[z, h, c].astype(F32) - rate * (tin[h] + xr[...].astype(F32))
    new_before = wp[...].astype(F32) - rate_before * (yi[...].astype(F32) + xp[...].astype(F32))
    o_in[...] = chosen(new_before, new)

    for off in NEAR:
        if off in (1, -1, 2, -2):
            win_out(off).wait_send()
        else:
            win_on(1 if off > 0 else -1, off).wait_send()
        win_x(off).wait_send()
    win_x(0).wait_send()
    prior.wait_send()
    cross_y.wait_send()
    for p in range(Q):
        next_out(p).wait_send()
    xwh.wait_send()
    cross.wait_send()
    head_y.wait_send()
    in_y.wait_send()
    for i in range(8):
        core_copy(core_off[i], i).wait_send()
    head_core.wait_send()
    sight_x.wait_send()
    sight_core.wait_send()
    sight_on.wait_send()
    core_sum.wait_send()
    for t in (1, 2, 3):
        quarter(t).wait_send()
        raw_out(mate(t)).wait_send()
        gr_out(t).wait_send()
        dh_mate(t).wait_send()
        out_mate(mate(t)).wait_send()
    for k in range(1, K):
        for way in (RIGHT, LEFT):
            for j in range(2):
                for kind in MID:
                    ag(kind, way, k, j).wait_send()
                ri_copy(way, k, j).wait_send()
            for p in range(Q):
                rs_copy(way, k, p).wait_send()
    for kind in MID:
        ag(kind, RIGHT, K, 0).wait_send()
        ag(kind, LEFT, K, 1).wait_send()
    ri_copy(RIGHT, K, 0).wait_send()
    ri_copy(LEFT, K, 1).wait_send()
    for j in range(2):
        rs_copy(RIGHT, K, j).wait_send()
        rs_copy(LEFT, K, 2 + j).wait_send()
    for off in (1, -1, 2, -2):
        dh_out(off).wait_send()
    for off in (3, -3, K):
        dh_on(1 if off > 0 else -1, off).wait_send()


def local(observations, returns, actions, w_input, w_middle, w_head, log_rate, copy_from, perturb):
    hbm = pl.BlockSpec(memory_space=pltpu.HBM)
    vmem = pl.BlockSpec(memory_space=pltpu.VMEM)
    smem = pl.BlockSpec(memory_space=pltpu.SMEM)
    V = pltpu.VMEM
    S = pltpu.SemaphoreType.DMA
    out = pl.pallas_call(
        kernel,
        out_shape=(
            jax.ShapeDtypeStruct((8, D), BF16),
            jax.ShapeDtypeStruct((64, D), BF16),
            jax.ShapeDtypeStruct((ACT, 64), BF16),
            jax.ShapeDtypeStruct((1,), F32),
            jax.ShapeDtypeStruct((1,), F32),
        ),
        in_specs=[hbm, vmem, vmem, hbm, hbm, hbm, smem, smem, smem],
        out_specs=(vmem, vmem, vmem, smem, smem),
        scratch_shapes=[
            V((Q, ROWS, OBS), BF16),
            V((OBS, D), BF16),
            V((Z, 2, 2, 8, D), BF16),
            V((Z, 2, 2, ACT, 64), BF16),
            V((Z, Q, 64, QC), BF16),
            V((D, OBS), BF16),
            V((QC, BK), BF16),
            V((D, OBS), F32),
            V((D, D), BF16),
            V((D, D), BF16),
            V((QC, D), F32),
            V((QC, D), BF16),
            V((QC, D), BF16),
            V((128, QC), F32),
            V((QC, 128), BF16),
            V((32, QC), BF16),
            V((Q, 24, ROWS), F32),
            V((Q, 24, ROWS), F32),
            V((Q, 32, ROWS), BF16),
            V((Z, Q, 64, QC), F32),
            V((2, K, Q, 64, QC), BF16),
            V((2, K, Q, 64, QC), BF16),
            V((Z, 2, 2, 8, D), F32),
            V((Z, 2, 8, D), BF16),
            V((Z, 2, 8, D), BF16),
            V((2, K, 2, 8, D), BF16),
            V((2, K, 2, 8, D), BF16),
            V((2, 8, D), F32),
            V((8, D), BF16),
            V((8, D), BF16),
            V((8, D), BF16),
            V((8, D), BF16),
            V((Z, 24, QC), BF16),
            V((Q, 24, QC), F32),
            V((QC, 24), F32),
            V((Q, 64, QC), BF16),
            V((Q, 64, QC), BF16),
            V((Q, 64, QC), BF16),
            V((8, D), BF16),
            V((8, D), BF16),
            V((ACT, 64), BF16),
            V((ACT, 64), BF16),
            S((2, 2, K, 2)), S((2, 2, K, 2)),
            S((7,)), S((7,)),
            S((8,)), S((8,)),
            S((6, Q)), S((6, Q)),
            S((3,)), S((3,)),
            S((10,)), S((10,)),
            S((7,)), S((7,)),
            S((2, K, Q)), S((2, K, Q)),
            S((2, K, 2)), S((2, K, 2)),
            S((7,)), S((7,)),
            S((4,)),
        ],
        compiler_params=pltpu.CompilerParams(
            collective_id=0, has_side_effects=True, vmem_limit_bytes=64 * 1024 * 1024 - 65536
        ),
    )(observations[0], returns, actions, w_input[0], w_middle[0], w_head[0].T, log_rate, copy_from, perturb)
    return out[0][None], out[1][None], out[2].T[None], out[3], out[4]


def solution(mesh):
    in_specs = (
        P("pop", "dp", None),
        P("pop", "dp"),
        P("pop", "dp"),
        P("pop", "dp", None),
        P("pop", "dp", None),
        P("pop", "dp", None),
        P(),
        P(),
        P(),
    )
    out_specs = (
        P("pop", "dp", None),
        P("pop", "dp", None),
        P("pop", "dp", None),
        P("pop"),
        P("pop"),
    )
    return jax.shard_map(local, mesh=mesh, in_specs=in_specs, out_specs=out_specs, check_vma=False)
```

```python
import jax
import jax.numpy as jnp
from jax import lax
from jax.experimental import pallas as pl
from jax.experimental.pallas import tpu as pltpu
from jax.sharding import PartitionSpec as P

F32 = jnp.float32
BF16 = jnp.bfloat16
Z = 8
K = Z // 2
Q = 4
ROWS = 512
OBS = 256
D = 2048
QC = D // Q
BK = D // Z
ACT = 18
POP = 8
BATCH = ROWS * Z * Q
WM, WH = 0, 1
OB, QT, RAW, GR, DH, OUT = range(6)
RIGHT, LEFT = 0, 1
NEAR = (1, -1, 2, -2, 3, -3, K)


def nt(a, b):
    return lax.dot_general(a, b, (((1,), (1,)), ((), ())), preferred_element_type=F32)


def nn(a, b):
    return jnp.dot(a, b, preferred_element_type=F32)


def kernel(
    obs, ret, act, win, wmid, whead, lrate, copyf, pert,
    o_in, o_mid, o_head, o_rate, o_fit,
    ob, obT, wi, wh, wq, w1T, wT, dT, h1, s1, p2, h2, g2, whp, whq, whT,
    raw_s, raw_r, gr, dW, rss, rsb, dI, sib_s, sib_r, ris, rib, tin, xs, xr,
    xp, wp, dH, dHg, tH, nm, ym, om, ni, yi, nh, yh,
    ag_s, ag_r, wz_s, wz_r, wx_s, wx_r, gp_s, gp_r, xp_s, xp_r, sb_s, sb_r, dh_s, dh_r, rs_s, rs_r, ri_s, ri_r, y_s, y_r, loc,
):
    m = lax.axis_index("pop")
    d = lax.axis_index("dp")
    z = d // Q
    q = lax.rem(d, Q)
    h = q // 2
    c = lax.rem(q, 2)
    sib = {"dp": z * Q + h * 2 + (1 - c)}
    xpt = {"dp": z * Q + (1 - h) * 2 + c}
    side = [{"dp": lax.rem(z + 1, Z) * Q + q}, {"dp": lax.rem(z + Z - 1, Z) * Q + q}]
    after = {"pop": lax.rem(m + 1, POP)}
    m_after = lax.rem(m + 1, POP)
    m_before = lax.rem(m + POP - 1, POP)
    before = {"pop": m_before}

    def mate(t):
        return lax.rem(q + t, Q)

    def mate_id(t):
        return {"dp": z * Q + mate(t)}

    def at(off):
        return lax.rem(z + off + Z, Z)

    def column(off):
        return {"dp": at(off) * Q + q}

    def copy(src, dst, ss, rs, dev):
        return pltpu.make_async_remote_copy(
            src_ref=src, dst_ref=dst, send_sem=ss, recv_sem=rs, device_id=dev,
            device_id_type=pl.DeviceIdType.MESH,
        )

    fetch = [
        pltpu.make_async_copy(win, wi.at[z, h, c], loc.at[0]),
        pltpu.make_async_copy(wmid.at[:, pl.ds(pl.multiple_of(q * QC, QC), QC)], wq.at[z, q], loc.at[1]),
        pltpu.make_async_copy(whead, wh.at[z, h, c], loc.at[2]),
        pltpu.make_async_copy(obs, ob.at[q], loc.at[3]),
    ]
    for f in fetch:
        f.start()

    barrier = pltpu.get_barrier_semaphore()
    met = [mate_id(t) for t in (1, 2, 3)] + [after, before] + [column(off) for off in (2, -2, 1, -1)]
    for near in (m_after, m_before):
        met += [{"pop": near, "dp": z * Q + mate(t)} for t in (1, 2, 3)]
    for dev in met:
        pl.semaphore_signal(barrier, inc=1, device_id=dev, device_id_type=pl.DeviceIdType.MESH)
    pl.semaphore_wait(barrier, len(met))

    def win_out(off):
        i = NEAR.index(off)
        return copy(win, wi.at[z, h, c], wz_s.at[i], wz_r.at[i], column(off))

    def win_in(off):
        i = NEAR.index(off)
        ref = wi.at[at(-off), h, c]
        copy(ref, ref, wz_s.at[i], wz_r.at[i], xpt).wait_recv()

    def win_x(off):
        i = 7 if off == 0 else NEAR.index(off)
        ref = wi.at[at(-off), h, c]
        return copy(win if off == 0 else ref, ref, wx_s.at[i], wx_r.at[i], xpt)

    def win_x_in(off):
        i = 7 if off == 0 else NEAR.index(off)
        ref = wi.at[at(-off), 1 - h, c]
        copy(ref, ref, wx_s.at[i], wx_r.at[i], xpt).wait_recv()

    def win_on(step, off):
        i = NEAR.index(off)
        ref = wi.at[at(-2 * step), h, c]
        return copy(ref, ref, wz_s.at[i], wz_r.at[i], column(off - 2 * step))

    for off in (2, -2, 1, -1):
        win_out(off).start()
    win_x(0).start()
    prior = copy(win, wp, y_s.at[6], y_r.at[6], after)
    xwh = copy(whead, wh.at[z, h, c], xp_s.at[1], xp_r.at[1], xpt)

    def quarter(t):
        p = mate(t)
        return copy(
            wmid.at[:, pl.ds(pl.multiple_of(p * QC, QC), QC)], wq.at[z, q], gp_s.at[QT, p], gp_r.at[QT, q], mate_id(t)
        )

    x_mate = (1 - h) * 2 + c
    sight_x = copy(obs, ob.at[q], gp_s.at[OB, 0], gp_r.at[OB, q], xpt)
    sight_core = copy(obs, ob.at[q], gp_s.at[OB, 1], gp_r.at[OB, q], sib)
    sight_on = copy(ob.at[x_mate], ob.at[x_mate], gp_s.at[OB, 2], gp_r.at[OB, x_mate], sib)

    def quarter_in(p):
        copy(wq.at[z, p], wq.at[z, p], gp_s.at[QT, p], gp_r.at[QT, p], sib).wait_recv()

    for t in (1, 2, 3):
        quarter(t).start()
    xwh.start()
    sight_core.start()
    prior.start()
    p2[...] = jnp.zeros_like(p2)
    dT[...] = jnp.zeros_like(dT)

    def piece(kind, b, j):
        if kind == WM:
            return wq.at[b, pl.ds(2 * j, 2)]
        return wh.at[b, j, c]

    def ag(kind, way, k, j):
        b = at(1 - k) if way == RIGHT else at(k - 1)
        ref = piece(kind, b, j)
        return copy(ref, ref, ag_s.at[kind, way, k - 1, j], ag_r.at[kind, way, k - 1, j], side[way])

    def ag_in(kind, way, k, j):
        b = at(-k) if way == RIGHT else at(k)
        ref = piece(kind, b, j)
        copy(ref, ref, ag_s.at[kind, way, k - 1, j], ag_r.at[kind, way, k - 1, j], side[way]).wait_recv()

    def put(kinds, k, j):
        for kind in kinds:
            for way in (RIGHT, LEFT):
                ag(kind, way, k, j).start()

    def take(kinds, k, j):
        for kind in kinds:
            for way in (RIGHT, LEFT):
                ag_in(kind, way, k, j)

    def take_last(kinds, k):
        for kind in kinds:
            ag_in(kind, RIGHT, k, 0)
            ag_in(kind, LEFT, k, 1)

    def put_last(kinds):
        for kind in kinds:
            ag(kind, RIGHT, K, 0).start()
            ag(kind, LEFT, K, 1).start()

    MID = (WM, WH)

    def core_copy(off, i):
        b = at(-off)
        return copy(wi.at[b, :, c], wi.at[b, :, c], sb_s.at[i], sb_r.at[i], sib)

    def core_in(off, i):
        b = at(-off)
        copy(wi.at[b, :, 1 - c], wi.at[b, :, 1 - c], sb_s.at[i], sb_r.at[i], sib).wait_recv()

    core_off = (0,) + NEAR
    head_core = copy(wh.at[:, :, c], wh.at[:, :, c], sb_s.at[9], sb_r.at[9], sib)

    def head_core_in():
        copy(wh.at[:, :, 1 - c], wh.at[:, :, 1 - c], sb_s.at[9], sb_r.at[9], sib).wait_recv()

    def obs_in(p):
        copy(ob.at[p], ob.at[p], gp_s.at[OB, 0], gp_r.at[OB, p], sib).wait_recv()

    def group_at(i):
        return (h + i // 2 * (1 - 2 * h)) * 2 + c + i % 2 * (1 - 2 * c)

    def turn_by(i, _):
        p = group_at(i)
        cols = pl.ds(pl.multiple_of(p * ROWS, ROWS), ROWS)
        obT[:, cols] = jnp.transpose(ob[p].astype(F32)).astype(BF16)
        return 0

    for off in NEAR[:2]:
        win_in(off)
        win_x(off).start()
    for off in NEAR[2:4]:
        win_in(off)
        win_on(off // 2, 3 * off // 2).start()
        if off > 0:
            win_on(1, K).start()
        win_x(off).start()
    fetch[1].wait()
    fetch[2].wait()
    quarter_in(h * 2 + (1 - c))
    put(MID, 1, h)
    quarter_in((1 - h) * 2)
    quarter_in((1 - h) * 2 + 1)
    xwh.wait_recv()
    put(MID, 1, 1 - h)
    fetch[3].wait()
    turn_by(0, 0)
    obs_in(h * 2 + (1 - c))
    turn_by(1, 0)
    for off in NEAR[4:]:
        win_in(off)
        win_x(off).start()
    sight_x.start()
    fetch[0].wait()
    for i, off in enumerate(core_off[:5]):
        win_x_in(off)
        core_copy(off, i).start()
    take(MID, 1, h)
    put(MID, 2, h)
    for i, off in enumerate(core_off[5:]):
        win_x_in(off)
        core_copy(off, 5 + i).start()
    take(MID, 1, 1 - h)
    put(MID, 2, 1 - h)
    for i in range(8):
        core_in(core_off[i], i)

    def turn_in(i, _):
        cols = pl.ds(pl.multiple_of(i * 256, 256), 256)
        x = wi[:, :, :, :, cols].astype(F32).reshape(OBS, 256)
        w1T[cols, :] = (0.5 * jnp.transpose(x)).astype(BF16)
        return 0

    lax.fori_loop(0, D // 256, turn_in, 0)

    def block_of(i):
        return at(((i + 1) // 2) * (2 * lax.rem(i + 1, 2) - 1))

    def first(i, p):
        feats = pl.ds(pl.multiple_of(i * BK, BK), BK)
        rows = pl.ds(pl.multiple_of(p * ROWS, ROWS), ROWS)
        u = nn(w1T[feats, :], obT[:, rows])
        t = jnp.tanh(u)
        a = 1.0 + t
        hid = u * a
        h1[feats, rows] = hid.astype(BF16)
        s1[feats, rows] = (a + hid * (1.0 - t)).astype(BF16)

    def block_rows(i):
        return pl.ds(pl.multiple_of(block_of(i) * BK, BK), BK)

    def turn_w(i):
        for b in range(2):
            x = wq[block_of(2 * i + b)].astype(F32).reshape(BK, QC)
            wT[b] = (0.5 * jnp.transpose(x)).astype(BF16)

    def second(i, rows):
        p2[:, rows] += nn(wT[0], h1[block_rows(2 * i), rows]) + nn(wT[1], h1[block_rows(2 * i + 1), rows])

    def first_by(i, _):
        @pl.when(i == 1)
        def _():
            with jax.named_scope("wait1"):
                take(MID, 2, h)
                put(MID, 3, h)

        @pl.when(i == 3)
        def _():
            with jax.named_scope("wait3"):
                obs_in(x_mate)
                sight_on.start()
                turn_by(2, 0)

        @pl.when(i == 4)
        def _():
            with jax.named_scope("wait4"):
                take(MID, 2, 1 - h)
                put(MID, 3, 1 - h)
                obs_in((1 - h) * 2 + (1 - c))
                turn_by(3, 0)

        @pl.when(i == 6)
        def _():
            with jax.named_scope("wait6"):
                take_last(MID, 3)
                put_last(MID)

        for b in range(2):
            for p in range(2):
                first(i % K * 2 + b, group_at(i // K * 2 + p))
        return 0

    def second_by(i, _):
        @pl.when(i == 2)
        def _():
            with jax.named_scope("wait2s"):
                for kind in MID:
                    ag_in(kind, RIGHT, 3, 1)
                    ag_in(kind, LEFT, 3, 0)

        turn_w(i)
        for p in range(Q):
            second(i, slice(p * ROWS, (p + 1) * ROWS))
        return 0

    lax.fori_loop(0, Z, first_by, 0)
    lax.fori_loop(0, K - 1, second_by, 0)
    take_last(MID, K)
    head_core.start()
    turn_w(K - 1)

    head_core_in()
    whp[...] = jnp.zeros_like(whp)
    for b in range(2):
        for i in range(Q):
            lanes = slice((b * Q + i) * 64, (b * Q + i + 1) * 64)
            whp[0:ACT, lanes] = wh[2 * q + b, i // 2, i % 2].astype(F32)
    whT[...] = whp[0:32, :].astype(BF16)
    whq[...] = jnp.transpose(whp[...]).astype(BF16)

    def raw_out(p):
        return copy(raw_s.at[p], raw_r.at[q], gp_s.at[RAW, p], gp_r.at[RAW, q], {"dp": z * Q + p})

    for t in (2, 1, 3, 0):
        p = mate(t)
        rows = pl.ds(pl.multiple_of(p * ROWS, ROWS), ROWS)

        second(K - 1, rows)

        def forward2(i, _):
            cols = pl.ds(pl.multiple_of(p * ROWS + i * 128, 128), 128)
            u = p2[:, cols]
            h2[:, cols] = (u + u * jnp.tanh(u)).astype(BF16)
            return 0

        lax.fori_loop(0, 4, forward2, 0)
        raw_s[p] = nn(whT[...], h2[:, rows])[0:24, :]
        if t:
            raw_out(p).start()
    def slope2(i, _):
        cols = pl.ds(pl.multiple_of(i * 128, 128), 128)
        u = p2[:, cols]
        t = jnp.tanh(u)
        a = 1.0 + t
        p2[:, cols] = a + u * a * (1.0 - t)
        return 0

    lax.fori_loop(0, D // 128, slope2, 0)
    raw = raw_s[q]
    for t in (2, 1, 3):
        p = mate(t)
        copy(raw_r.at[p], raw_r.at[p], gp_s.at[RAW, p], gp_r.at[RAW, p], sib).wait_recv()
        raw = raw + raw_r[p]
    at_act = lax.broadcasted_iota(jnp.int32, raw.shape, 0)
    squash = jnp.tanh(raw * 0.5)
    logits = 2.0 * squash
    e = jnp.where(at_act < ACT, jnp.exp(logits), 0.0)
    total = jnp.sum(e, axis=0, keepdims=True)
    logp = logits - jnp.log(total)
    onehot = jnp.where(at_act == act[...], 1.0, 0.0)
    gains = ret[...] * (1.0 / BATCH)
    term = gains * jnp.sum(logp * onehot, axis=0, keepdims=True)
    grad = -gains * (onehot - e / total) * (1.0 - squash * squash)
    high = term.astype(BF16).astype(F32)
    low = term - high
    grad = jnp.where(at_act < ACT, grad, jnp.where(at_act == ACT, high, jnp.where(at_act == ACT + 1, low, 0.0)))
    gr[q] = jnp.concatenate([grad, jnp.zeros((8, ROWS), F32)], axis=0).astype(BF16)

    def gr_out(t):
        return copy(gr.at[q], gr.at[q], gp_s.at[GR, mate(t)], gp_r.at[GR, q], mate_id(t))

    for t in (2, 1, 3):
        gr_out(t).start()
    wb = (0.5 * whq[:, 0:32].astype(F32)).astype(BF16)

    def grad2(i):
        p = group_at(i)
        if i:
            copy(gr.at[p], gr.at[p], gp_s.at[GR, p], gp_r.at[GR, p], sib).wait_recv()
        rows = pl.ds(pl.multiple_of(p * ROWS, ROWS), ROWS)
        g2[:, rows] = (nn(wb, gr[p]) * p2[:, rows]).astype(BF16)

    def back(i, _):
        p = group_at(i // 2)
        rows = pl.ds(pl.multiple_of(p * ROWS, ROWS), ROWS)
        half = lax.rem(i, 2)
        feats = pl.ds(pl.multiple_of(half * (D // 2), D // 2), D // 2)
        w = wq[pl.ds(half * (Z // 2), Z // 2)].reshape(D // 2, QC)
        g = (nn(w, g2[:, rows]) * s1[feats, rows].astype(F32)).astype(BF16)
        dT[feats, :] += nn(g, ob[p])
        return 0

    grad2(0)
    lax.fori_loop(0, 2, back, 0)
    grad2(1)
    grad2(2)
    grad2(3)

    def middle(i, _):
        one = at(K + i)
        two = at(K - 1 - i)
        at_one = pl.ds(pl.multiple_of(one * BK, BK), BK)
        at_two = pl.ds(pl.multiple_of(two * BK, BK), BK)
        both = nt(jnp.concatenate([h1[at_one, :], h1[at_two, :]], axis=0), g2[...])
        dW[one] = both[0:BK].reshape(Q, BK // Q, QC)
        dW[two] = both[BK:].reshape(Q, BK // Q, QC)
        return 0

    def rs_copy(way, k, p):
        return copy(
            rss.at[way, k - 1, p], rsb.at[way, k - 1, p], rs_s.at[way, k - 1, p], rs_r.at[way, k - 1, p], side[way]
        )

    def rs_in(way, k, p):
        copy(rsb.at[way, k, p], rsb.at[way, k, p], rs_s.at[way, k, p], rs_r.at[way, k, p], side[way]).wait_recv()
        return rsb[way, k, p].astype(F32)

    def rs_put(way, k, p, joined):
        v = dW[at(k if way == RIGHT else -k), p]
        if joined:
            v = v + rs_in(way, k, p)
        rss[way, k - 1, p] = v.astype(BF16)
        rs_copy(way, k, p).start()

    def rs_open(j, _):
        rs_put(RIGHT, K, j, False)
        rs_put(LEFT, K, 2 + j, False)
        return 0

    def rs_open2(j, _):
        rs_put(RIGHT, K - 1, 2 + j, False)
        rs_put(LEFT, K - 1, j, False)
        return 0

    def middle_open(i, _):
        middle(i, 0)

        @pl.when(i == 0)
        def _():
            lax.fori_loop(0, 2, rs_open, 0)

        return 0

    lax.fori_loop(0, 2, middle_open, 0)
    lax.fori_loop(0, 2, rs_open2, 0)

    acc = jnp.zeros((32, QC), F32)
    fit = jnp.zeros((1, ROWS), F32)
    for p in range(Q):
        acc = acc + nt(gr[p], h2[:, p * ROWS : (p + 1) * ROWS])
        x = gr[p].astype(F32)
        fit = fit + x[ACT : ACT + 1, :] + x[ACT + 1 : ACT + 2, :]
    at_head = lax.broadcasted_iota(jnp.int32, (24, QC), 0)
    fit_high = fit.astype(BF16).astype(F32)
    packed = jnp.where(at_head == ACT, fit_high, jnp.where(at_head == ACT + 1, fit - fit_high, acc[0:24, :]))
    dH[z] = packed.astype(BF16)

    def dh_out(off):
        i = NEAR.index(off)
        return copy(dH.at[z], dH.at[z], dh_s.at[i], dh_r.at[i], column(off))

    def dh_on(step, off):
        i = NEAR.index(off)
        ref = dH.at[at(-2 * step)]
        return copy(ref, ref, dh_s.at[i], dh_r.at[i], column(off - 2 * step))

    def dh_in(off):
        i = NEAR.index(off)
        ref = dH.at[at(-off)]
        copy(ref, ref, dh_s.at[i], dh_r.at[i], sib).wait_recv()

    for off in (2, -2, 1, -1):
        dh_out(off).start()

    def join3(j, _):
        rs_put(RIGHT, K - 1, j, True)
        rs_put(LEFT, K - 1, 2 + j, True)
        return 0

    def join2(j, _):
        rs_put(RIGHT, 2, lax.rem(2 + j, Q), True)
        rs_put(LEFT, 2, j, True)
        return 0

    lax.fori_loop(2, 4, back, 0)
    lax.fori_loop(0, 2, join3, 0)
    lax.fori_loop(4, 8, back, 0)

    def turn_back(i, _):
        feats = pl.ds(pl.multiple_of(i * 256, 256), 256)
        x = 0.5 * jnp.transpose(dT[feats, :])
        dI[:, :, :, :, feats] = x.reshape(Z, 2, 2, 8, 256)
        return 0

    dh_in(2)
    dh_on(1, 3).start()
    dh_on(1, K).start()
    dh_in(-2)
    dh_on(-1, -3).start()
    lax.fori_loop(0, Z, turn_back, 0)

    for b in range(Z):
        for j in range(2):
            sib_s[b, j] = dI[b, j, 1 - c].astype(BF16)
    core_sum = copy(sib_s, sib_r, sb_s.at[8], sb_r.at[8], sib)
    core_sum.start()
    lax.fori_loop(2, 3, middle, 0)
    core_sum.wait_recv()

    def own_in(off, j):
        b = at(off)
        return dI[b, j, c] + sib_r[b, j].astype(F32)

    def ri_copy(way, k, j):
        return copy(
            ris.at[way, k - 1, j], rib.at[way, k - 1, j], ri_s.at[way, k - 1, j], ri_r.at[way, k - 1, j], side[way]
        )

    def ri_in(way, k, j):
        copy(rib.at[way, k, j], rib.at[way, k, j], ri_s.at[way, k, j], ri_r.at[way, k, j], side[way]).wait_recv()
        return rib[way, k, j].astype(F32)

    def ri_put(way, k, j, joined):
        v = own_in(k if way == RIGHT else -k, j)
        if joined:
            v = v + ri_in(way, k, j)
        ris[way, k - 1, j] = v.astype(BF16)
        ri_copy(way, k, j).start()

    ri_put(RIGHT, 4, 0, False)
    ri_put(LEFT, 4, 1, False)
    ri_put(RIGHT, 3, 1, False)
    ri_put(LEFT, 3, 0, False)

    lr = lrate[m]
    lr_before = lrate[m_before]
    rate = jnp.exp(jnp.full((8, 128), lr, F32))[0:1, 0:1]
    rate_before = jnp.exp(jnp.full((8, 128), lr_before, F32))[0:1, 0:1]
    flag = copyf[m]

    def next_out(p):
        return copy(nm.at[p], ym.at[q], y_s.at[p], y_r.at[q], {"pop": m_after, "dp": z * Q + p})

    def out_mate(p):
        return copy(nm.at[p], om.at[q], gp_s.at[OUT, p], gp_r.at[OUT, q], {"dp": z * Q + p})

    def middle_end(p):
        g = dW[z, p] + rs_in(RIGHT, 0, p) + rs_in(LEFT, 0, p)
        nm[p] = (wq[z, p].astype(F32) - rate * g).astype(BF16)
        next_out(p).start()

        @pl.when(p != q)
        def _():
            out_mate(p).start()

    def ones(j, _):
        rs_put(RIGHT, 1, lax.rem(2 + j, Q), True)
        rs_put(LEFT, 1, j, True)
        return 0

    lax.fori_loop(0, 2, join2, 0)
    lax.fori_loop(3, 4, middle, 0)
    ri_put(RIGHT, 3, 0, True)
    ri_put(LEFT, 3, 1, True)
    lax.fori_loop(2, 4, join2, 0)
    for j in range(2):
        ri_put(RIGHT, 2, j, True)
        ri_put(LEFT, 2, j, True)
    lax.fori_loop(0, 2, ones, 0)
    lax.fori_loop(2, 4, ones, 0)
    for off in (1, -1, 3, -3, K):
        dh_in(off)
    tot = dH[0].astype(F32)
    for b in range(1, Z):
        tot = tot + dH[b].astype(F32)
    dHg[q] = tot
    o_fit[0] = jnp.sum(tot[ACT : ACT + 2, :])

    def dh_mate(t):
        return copy(dHg.at[q], dHg.at[q], gp_s.at[DH, mate(t)], gp_r.at[DH, q], mate_id(t))

    for t in (2, 1, 3):
        dh_mate(t).start()

    for j in range(2):
        ri_put(RIGHT, 1, j, True)
        ri_put(LEFT, 1, j, True)
    for t in (2, 1, 3):
        p = mate(t)
        copy(dHg.at[p], dHg.at[p], gp_s.at[DH, p], gp_r.at[DH, p], sib).wait_recv()
    tH[...] = jnp.transpose(dHg[z // 2])
    own_rows = pl.ds(pl.multiple_of(lax.rem(d, Z) * 64, 64), 64)
    nh[...] = (wh[z, h, c].astype(F32) - rate * jnp.transpose(tH[own_rows, :])[0:ACT, :]).astype(BF16)
    head_y = copy(nh, yh, y_s.at[5], y_r.at[5], after)
    head_y.start()
    middle_end(0)
    middle_end(2)
    middle_end(1)
    middle_end(3)
    for j in range(2):
        tin[j] = own_in(0, j) + ri_in(RIGHT, 0, j) + ri_in(LEFT, 0, j)
    xs[...] = tin[1 - h].astype(BF16)
    cross = copy(xs, xr, xp_s.at[2], xp_r.at[2], xpt)
    cross.start()
    cross_y = copy(xs, xp, xp_s.at[0], xp_r.at[0], {"pop": m_after, "dp": xpt["dp"]})
    cross_y.start()
    ni[...] = tin[h].astype(BF16)
    in_y = copy(ni, yi, y_s.at[4], y_r.at[4], after)
    in_y.start()
    def chosen(got, own):
        return jnp.where(jnp.full(own.shape, flag) == 1, got.astype(F32), own.astype(F32)).astype(BF16)

    head_y.wait_recv()
    o_head[...] = chosen(yh[...], nh[...])
    for t in (0, 1, 2, 3):
        p = mate(t)
        own = nm.at[p] if t == 0 else om.at[p]
        if t:
            copy(own, own, gp_s.at[OUT, p], gp_r.at[OUT, p], sib).wait_recv()
        copy(ym.at[p], ym.at[p], y_s.at[p], y_r.at[p], after).wait_recv()
        o_mid[:, pl.ds(pl.multiple_of(p * QC, QC), QC)] = chosen(ym[p], own[...])
    pick = pert[m]
    o_rate[0] = jnp.where(flag == 1, lr_before, lr) + jnp.where(pick == 0, -0.2, jnp.where(pick == 1, 0.0, 0.2))
    prior.wait_recv()
    cross.wait_recv()
    cross_y.wait_recv()
    in_y.wait_recv()
    new = wi[z, h, c].astype(F32) - rate * (tin[h] + xr[...].astype(F32))
    new_before = wp[...].astype(F32) - rate_before * (yi[...].astype(F32) + xp[...].astype(F32))
    o_in[...] = chosen(new_before, new)

    for off in NEAR:
        if off in (1, -1, 2, -2):
            win_out(off).wait_send()
        else:
            win_on(1 if off > 0 else -1, off).wait_send()
        win_x(off).wait_send()
    win_x(0).wait_send()
    prior.wait_send()
    cross_y.wait_send()
    for p in range(Q):
        next_out(p).wait_send()
    xwh.wait_send()
    cross.wait_send()
    head_y.wait_send()
    in_y.wait_send()
    for i in range(8):
        core_copy(core_off[i], i).wait_send()
    head_core.wait_send()
    sight_x.wait_send()
    sight_core.wait_send()
    sight_on.wait_send()
    core_sum.wait_send()
    for t in (1, 2, 3):
        quarter(t).wait_send()
        raw_out(mate(t)).wait_send()
        gr_out(t).wait_send()
        dh_mate(t).wait_send()
        out_mate(mate(t)).wait_send()
    for k in range(1, K):
        for way in (RIGHT, LEFT):
            for j in range(2):
                for kind in MID:
                    ag(kind, way, k, j).wait_send()
                ri_copy(way, k, j).wait_send()
            for p in range(Q):
                rs_copy(way, k, p).wait_send()
    for kind in MID:
        ag(kind, RIGHT, K, 0).wait_send()
        ag(kind, LEFT, K, 1).wait_send()
    ri_copy(RIGHT, K, 0).wait_send()
    ri_copy(LEFT, K, 1).wait_send()
    for j in range(2):
        rs_copy(RIGHT, K, j).wait_send()
        rs_copy(LEFT, K, 2 + j).wait_send()
    for off in (1, -1, 2, -2):
        dh_out(off).wait_send()
    for off in (3, -3, K):
        dh_on(1 if off > 0 else -1, off).wait_send()


def local(observations, returns, actions, w_input, w_middle, w_head, log_rate, copy_from, perturb):
    hbm = pl.BlockSpec(memory_space=pltpu.HBM)
    vmem = pl.BlockSpec(memory_space=pltpu.VMEM)
    smem = pl.BlockSpec(memory_space=pltpu.SMEM)
    V = pltpu.VMEM
    S = pltpu.SemaphoreType.DMA
    out = pl.pallas_call(
        kernel,
        out_shape=(
            pltpu.VMEM((8, D), BF16),
            pltpu.VMEM((64, D), BF16),
            pltpu.VMEM((ACT, 64), BF16),
            jax.ShapeDtypeStruct((1,), F32),
            jax.ShapeDtypeStruct((1,), F32),
        ),
        in_specs=[hbm, vmem, vmem, hbm, hbm, hbm, smem, smem, smem],
        out_specs=(vmem, vmem, vmem, smem, smem),
        scratch_shapes=[
            V((Q, ROWS, OBS), BF16),
            V((OBS, D), BF16),
            V((Z, 2, 2, 8, D), BF16),
            V((Z, 2, 2, ACT, 64), BF16),
            V((Z, Q, 64, QC), BF16),
            V((D, OBS), BF16),
            V((2, QC, BK), BF16),
            V((D, OBS), F32),
            V((D, D), BF16),
            V((D, D), BF16),
            V((QC, D), F32),
            V((QC, D), BF16),
            V((QC, D), BF16),
            V((128, QC), F32),
            V((QC, 128), BF16),
            V((32, QC), BF16),
            V((Q, 24, ROWS), F32),
            V((Q, 24, ROWS), F32),
            V((Q, 32, ROWS), BF16),
            V((Z, Q, 64, QC), F32),
            V((2, K, Q, 64, QC), BF16),
            V((2, K, Q, 64, QC), BF16),
            V((Z, 2, 2, 8, D), F32),
            V((Z, 2, 8, D), BF16),
            V((Z, 2, 8, D), BF16),
            V((2, K, 2, 8, D), BF16),
            V((2, K, 2, 8, D), BF16),
            V((2, 8, D), F32),
            V((8, D), BF16),
            V((8, D), BF16),
            V((8, D), BF16),
            V((8, D), BF16),
            V((Z, 24, QC), BF16),
            V((Q, 24, QC), F32),
            V((QC, 24), F32),
            V((Q, 64, QC), BF16),
            V((Q, 64, QC), BF16),
            V((Q, 64, QC), BF16),
            V((8, D), BF16),
            V((8, D), BF16),
            V((ACT, 64), BF16),
            V((ACT, 64), BF16),
            S((2, 2, K, 2)), S((2, 2, K, 2)),
            S((7,)), S((7,)),
            S((8,)), S((8,)),
            S((6, Q)), S((6, Q)),
            S((3,)), S((3,)),
            S((10,)), S((10,)),
            S((7,)), S((7,)),
            S((2, K, Q)), S((2, K, Q)),
            S((2, K, 2)), S((2, K, 2)),
            S((7,)), S((7,)),
            S((4,)),
        ],
        compiler_params=pltpu.CompilerParams(
            collective_id=0, has_side_effects=True, vmem_limit_bytes=60 * 1024 * 1024
        ),
    )(observations[0], returns, actions, w_input[0], w_middle[0], w_head[0].T, log_rate, copy_from, perturb)
    return out[0][None], out[1][None], out[2].T[None], out[3], out[4]


def solution(mesh):
    in_specs = (
        P("pop", "dp", None),
        P("pop", "dp"),
        P("pop", "dp"),
        P("pop", "dp", None),
        P("pop", "dp", None),
        P("pop", "dp", None),
        P(),
        P(),
        P(),
    )
    out_specs = (
        P("pop", "dp", None),
        P("pop", "dp", None),
        P("pop", "dp", None),
        P("pop"),
        P("pop"),
    )
    return jax.shard_map(local, mesh=mesh, in_specs=in_specs, out_specs=out_specs, check_vma=False)
```

```python
import jax
import jax.numpy as jnp
from jax import lax
from jax.experimental import pallas as pl
from jax.experimental.pallas import tpu as pltpu
from jax.sharding import PartitionSpec as P

F32 = jnp.float32
BF16 = jnp.bfloat16
Z = 8
K = Z // 2
Q = 4
ROWS = 512
OBS = 256
D = 2048
QC = D // Q
BK = D // Z
ACT = 18
POP = 8
BATCH = ROWS * Z * Q
WM, WH = 0, 1
OB, QT, RAW, GR, DH, OUT = range(6)
RIGHT, LEFT = 0, 1
NEAR = (1, -1, 2, -2, 3, -3, K)


def nt(a, b):
    return lax.dot_general(a, b, (((1,), (1,)), ((), ())), preferred_element_type=F32)


def nn(a, b):
    return jnp.dot(a, b, preferred_element_type=F32)


def kernel(
    obs, ret, act, win, wmid, whead, lrate, copyf, pert,
    o_in, o_mid, o_head, o_rate, o_fit,
    ob, obT, wi, wh, wq, w1T, wT, dT, h1, s1, p2, h2, g2, whp, whq, whT,
    raw_s, raw_r, gr, dW, rss, rsb, dI, sib_s, sib_r, ris, rib, tin, xs, xr,
    xp, wp, dH, dHg, tH, nm, ym, om, ni, yi, nh, yh,
    ag_s, ag_r, wz_s, wz_r, wx_s, wx_r, gp_s, gp_r, xp_s, xp_r, sb_s, sb_r, dh_s, dh_r, rs_s, rs_r, ri_s, ri_r, y_s, y_r, loc,
):
    m = lax.axis_index("pop")
    d = lax.axis_index("dp")
    z = d // Q
    q = lax.rem(d, Q)
    h = q // 2
    c = lax.rem(q, 2)
    sib = {"dp": z * Q + h * 2 + (1 - c)}
    xpt = {"dp": z * Q + (1 - h) * 2 + c}
    side = [{"dp": lax.rem(z + 1, Z) * Q + q}, {"dp": lax.rem(z + Z - 1, Z) * Q + q}]
    after = {"pop": lax.rem(m + 1, POP)}
    m_after = lax.rem(m + 1, POP)
    m_before = lax.rem(m + POP - 1, POP)
    before = {"pop": m_before}

    def mate(t):
        return lax.rem(q + t, Q)

    def mate_id(t):
        return {"dp": z * Q + mate(t)}

    def at(off):
        return lax.rem(z + off + Z, Z)

    def column(off):
        return {"dp": at(off) * Q + q}

    def copy(src, dst, ss, rs, dev):
        return pltpu.make_async_remote_copy(
            src_ref=src, dst_ref=dst, send_sem=ss, recv_sem=rs, device_id=dev,
            device_id_type=pl.DeviceIdType.MESH,
        )

    fetch = [
        pltpu.make_async_copy(win, wi.at[z, h, c], loc.at[0]),
        pltpu.make_async_copy(wmid.at[:, pl.ds(pl.multiple_of(q * QC, QC), QC)], wq.at[z, q], loc.at[1]),
        pltpu.make_async_copy(whead, wh.at[z, h, c], loc.at[2]),
        pltpu.make_async_copy(obs, ob.at[q], loc.at[3]),
    ]
    for f in fetch:
        f.start()

    barrier = pltpu.get_barrier_semaphore()
    met = [mate_id(t) for t in (1, 2, 3)] + [after, before] + [column(off) for off in (2, -2, 1, -1)]
    for near in (m_after, m_before):
        met += [{"pop": near, "dp": z * Q + mate(t)} for t in (1, 2, 3)]
    for dev in met:
        pl.semaphore_signal(barrier, inc=1, device_id=dev, device_id_type=pl.DeviceIdType.MESH)
    pl.semaphore_wait(barrier, len(met))

    def win_out(off):
        i = NEAR.index(off)
        return copy(win, wi.at[z, h, c], wz_s.at[i], wz_r.at[i], column(off))

    def win_in(off):
        i = NEAR.index(off)
        ref = wi.at[at(-off), h, c]
        copy(ref, ref, wz_s.at[i], wz_r.at[i], xpt).wait_recv()

    def win_x(off):
        i = 7 if off == 0 else NEAR.index(off)
        ref = wi.at[at(-off), h, c]
        return copy(win if off == 0 else ref, ref, wx_s.at[i], wx_r.at[i], xpt)

    def win_x_in(off):
        i = 7 if off == 0 else NEAR.index(off)
        ref = wi.at[at(-off), 1 - h, c]
        copy(ref, ref, wx_s.at[i], wx_r.at[i], xpt).wait_recv()

    def win_on(step, off):
        i = NEAR.index(off)
        ref = wi.at[at(-2 * step), h, c]
        return copy(ref, ref, wz_s.at[i], wz_r.at[i], column(off - 2 * step))

    for off in (2, -2, 1, -1):
        win_out(off).start()
    win_x(0).start()
    prior = copy(win, wp, y_s.at[6], y_r.at[6], after)
    xwh = copy(whead, wh.at[z, h, c], xp_s.at[1], xp_r.at[1], xpt)

    def quarter(t):
        p = mate(t)
        return copy(
            wmid.at[:, pl.ds(pl.multiple_of(p * QC, QC), QC)], wq.at[z, q], gp_s.at[QT, p], gp_r.at[QT, q], mate_id(t)
        )

    x_mate = (1 - h) * 2 + c
    sight_x = copy(obs, ob.at[q], gp_s.at[OB, 0], gp_r.at[OB, q], xpt)
    sight_core = copy(obs, ob.at[q], gp_s.at[OB, 1], gp_r.at[OB, q], sib)
    sight_on = copy(ob.at[x_mate], ob.at[x_mate], gp_s.at[OB, 2], gp_r.at[OB, x_mate], sib)

    def quarter_in(p):
        copy(wq.at[z, p], wq.at[z, p], gp_s.at[QT, p], gp_r.at[QT, p], sib).wait_recv()

    for t in (1, 2, 3):
        quarter(t).start()
    xwh.start()
    sight_core.start()
    prior.start()
    p2[...] = jnp.zeros_like(p2)
    dT[...] = jnp.zeros_like(dT)

    def piece(kind, b, j):
        if kind == WM:
            return wq.at[b, pl.ds(2 * j, 2)]
        return wh.at[b, j, c]

    def ag(kind, way, k, j):
        b = at(1 - k) if way == RIGHT else at(k - 1)
        ref = piece(kind, b, j)
        return copy(ref, ref, ag_s.at[kind, way, k - 1, j], ag_r.at[kind, way, k - 1, j], side[way])

    def ag_in(kind, way, k, j):
        b = at(-k) if way == RIGHT else at(k)
        ref = piece(kind, b, j)
        copy(ref, ref, ag_s.at[kind, way, k - 1, j], ag_r.at[kind, way, k - 1, j], side[way]).wait_recv()

    def put(kinds, k, j):
        for kind in kinds:
            for way in (RIGHT, LEFT):
                ag(kind, way, k, j).start()

    def take(kinds, k, j):
        for kind in kinds:
            for way in (RIGHT, LEFT):
                ag_in(kind, way, k, j)

    def take_last(kinds, k):
        for kind in kinds:
            ag_in(kind, RIGHT, k, 0)
            ag_in(kind, LEFT, k, 1)

    def put_last(kinds):
        for kind in kinds:
            ag(kind, RIGHT, K, 0).start()
            ag(kind, LEFT, K, 1).start()

    MID = (WM, WH)

    def core_copy(off, i):
        b = at(-off)
        return copy(wi.at[b, :, c], wi.at[b, :, c], sb_s.at[i], sb_r.at[i], sib)

    def core_in(off, i):
        b = at(-off)
        copy(wi.at[b, :, 1 - c], wi.at[b, :, 1 - c], sb_s.at[i], sb_r.at[i], sib).wait_recv()

    core_off = (0,) + NEAR
    head_core = copy(wh.at[:, :, c], wh.at[:, :, c], sb_s.at[9], sb_r.at[9], sib)

    def head_core_in():
        copy(wh.at[:, :, 1 - c], wh.at[:, :, 1 - c], sb_s.at[9], sb_r.at[9], sib).wait_recv()

    def obs_in(p):
        copy(ob.at[p], ob.at[p], gp_s.at[OB, 0], gp_r.at[OB, p], sib).wait_recv()

    def group_at(i):
        return (h + i // 2 * (1 - 2 * h)) * 2 + c + i % 2 * (1 - 2 * c)

    def turn_by(i, _):
        p = group_at(i)
        cols = pl.ds(pl.multiple_of(p * ROWS, ROWS), ROWS)
        obT[:, cols] = jnp.transpose(ob[p].astype(F32)).astype(BF16)
        return 0

    for off in NEAR[:2]:
        win_in(off)
        win_x(off).start()
    for off in NEAR[2:4]:
        win_in(off)
        win_on(off // 2, 3 * off // 2).start()
        if off > 0:
            win_on(1, K).start()
        win_x(off).start()
    fetch[1].wait()
    fetch[2].wait()
    quarter_in(h * 2 + (1 - c))
    put(MID, 1, h)
    quarter_in((1 - h) * 2)
    quarter_in((1 - h) * 2 + 1)
    xwh.wait_recv()
    put(MID, 1, 1 - h)
    fetch[3].wait()
    turn_by(0, 0)
    obs_in(h * 2 + (1 - c))
    turn_by(1, 0)
    for off in NEAR[4:]:
        win_in(off)
        win_x(off).start()
    sight_x.start()
    fetch[0].wait()
    for i, off in enumerate(core_off[:5]):
        win_x_in(off)
        core_copy(off, i).start()
    take(MID, 1, h)
    put(MID, 2, h)
    for i, off in enumerate(core_off[5:]):
        win_x_in(off)
        core_copy(off, 5 + i).start()
    take(MID, 1, 1 - h)
    put(MID, 2, 1 - h)
    for i in range(8):
        core_in(core_off[i], i)

    def turn_in(i, _):
        cols = pl.ds(pl.multiple_of(i * 256, 256), 256)
        x = wi[:, :, :, :, cols].astype(F32).reshape(OBS, 256)
        w1T[cols, :] = (0.5 * jnp.transpose(x)).astype(BF16)
        return 0

    lax.fori_loop(0, D // 256, turn_in, 0)

    def block_of(i):
        return at(((i + 1) // 2) * (2 * lax.rem(i + 1, 2) - 1))

    def first(i, p):
        feats = pl.ds(pl.multiple_of(i * BK, BK), BK)
        rows = pl.ds(pl.multiple_of(p * ROWS, ROWS), ROWS)
        u = nn(w1T[feats, :], obT[:, rows])
        t = jnp.tanh(u)
        a = 1.0 + t
        hid = u * a
        h1[feats, rows] = hid.astype(BF16)
        s1[feats, rows] = (a + hid * (1.0 - t)).astype(BF16)

    def block_rows(i):
        return pl.ds(pl.multiple_of(block_of(i) * BK, BK), BK)

    def turn_w(i):
        for b in range(2):
            x = wq[block_of(2 * i + b)].astype(F32).reshape(BK, QC)
            wT[b] = (0.5 * jnp.transpose(x)).astype(BF16)

    def second(i, rows):
        p2[:, rows] += nn(wT[0], h1[block_rows(2 * i), rows]) + nn(wT[1], h1[block_rows(2 * i + 1), rows])

    def first_by(i, _):
        @pl.when(i == 1)
        def _():
            with jax.named_scope("wait1"):
                take(MID, 2, h)
                put(MID, 3, h)

        @pl.when(i == 3)
        def _():
            with jax.named_scope("wait3"):
                obs_in(x_mate)
                sight_on.start()
                turn_by(2, 0)

        @pl.when(i == 4)
        def _():
            with jax.named_scope("wait4"):
                take(MID, 2, 1 - h)
                put(MID, 3, 1 - h)
                obs_in((1 - h) * 2 + (1 - c))
                turn_by(3, 0)

        @pl.when(i == 6)
        def _():
            with jax.named_scope("wait6"):
                take_last(MID, 3)
                put_last(MID)

        for b in range(2):
            for p in range(2):
                first(i % K * 2 + b, group_at(i // K * 2 + p))
        return 0

    def second_by(i, _):
        @pl.when(i == 2)
        def _():
            with jax.named_scope("wait2s"):
                for kind in MID:
                    ag_in(kind, RIGHT, 3, 1)
                    ag_in(kind, LEFT, 3, 0)
                take_last(MID, K)
                head_core.start()

        turn_w(i)
        for p in range(Q):
            second(i, slice(p * ROWS, (p + 1) * ROWS))
        return 0

    lax.fori_loop(0, Z, first_by, 0)
    lax.fori_loop(0, K - 1, second_by, 0)
    turn_w(K - 1)

    head_core_in()
    whp[...] = jnp.zeros_like(whp)
    for b in range(2):
        for i in range(Q):
            lanes = slice((b * Q + i) * 64, (b * Q + i + 1) * 64)
            whp[0:ACT, lanes] = wh[2 * q + b, i // 2, i % 2].astype(F32)
    whT[...] = whp[0:32, :].astype(BF16)
    whq[...] = jnp.transpose(whp[...]).astype(BF16)

    def raw_out(p):
        return copy(raw_s.at[p], raw_r.at[q], gp_s.at[RAW, p], gp_r.at[RAW, q], {"dp": z * Q + p})

    for t in (2, 1, 3, 0):
        p = mate(t)
        rows = pl.ds(pl.multiple_of(p * ROWS, ROWS), ROWS)

        second(K - 1, rows)

        def forward2(i, _):
            cols = pl.ds(pl.multiple_of(p * ROWS + i * 128, 128), 128)
            u = p2[:, cols]
            h2[:, cols] = (u + u * jnp.tanh(u)).astype(BF16)
            return 0

        lax.fori_loop(0, 4, forward2, 0)
        raw_s[p] = nn(whT[...], h2[:, rows])[0:24, :]
        if t:
            raw_out(p).start()
    def slope2(i, _):
        cols = pl.ds(pl.multiple_of(i * 128, 128), 128)
        u = p2[:, cols]
        t = jnp.tanh(u)
        a = 1.0 + t
        p2[:, cols] = a + u * a * (1.0 - t)
        return 0

    lax.fori_loop(0, D // 128, slope2, 0)
    raw = raw_s[q]
    for t in (2, 1, 3):
        p = mate(t)
        copy(raw_r.at[p], raw_r.at[p], gp_s.at[RAW, p], gp_r.at[RAW, p], sib).wait_recv()
        raw = raw + raw_r[p]
    at_act = lax.broadcasted_iota(jnp.int32, raw.shape, 0)
    squash = jnp.tanh(raw * 0.5)
    logits = 2.0 * squash
    e = jnp.where(at_act < ACT, jnp.exp(logits), 0.0)
    total = jnp.sum(e, axis=0, keepdims=True)
    logp = logits - jnp.log(total)
    onehot = jnp.where(at_act == act[...], 1.0, 0.0)
    gains = ret[...] * (1.0 / BATCH)
    term = gains * jnp.sum(logp * onehot, axis=0, keepdims=True)
    grad = -gains * (onehot - e / total) * (1.0 - squash * squash)
    high = term.astype(BF16).astype(F32)
    low = term - high
    grad = jnp.where(at_act < ACT, grad, jnp.where(at_act == ACT, high, jnp.where(at_act == ACT + 1, low, 0.0)))
    gr[q] = jnp.concatenate([grad, jnp.zeros((8, ROWS), F32)], axis=0).astype(BF16)

    def gr_out(t):
        return copy(gr.at[q], gr.at[q], gp_s.at[GR, mate(t)], gp_r.at[GR, q], mate_id(t))

    for t in (2, 1, 3):
        gr_out(t).start()
    wb = (0.5 * whq[:, 0:32].astype(F32)).astype(BF16)

    def grad2(i):
        p = group_at(i)
        if i:
            copy(gr.at[p], gr.at[p], gp_s.at[GR, p], gp_r.at[GR, p], sib).wait_recv()
        rows = pl.ds(pl.multiple_of(p * ROWS, ROWS), ROWS)
        g2[:, rows] = (nn(wb, gr[p]) * p2[:, rows]).astype(BF16)

    def back(i, _):
        p = group_at(i // 2)
        rows = pl.ds(pl.multiple_of(p * ROWS, ROWS), ROWS)
        half = lax.rem(i, 2)
        feats = pl.ds(pl.multiple_of(half * (D // 2), D // 2), D // 2)
        w = wq[pl.ds(half * (Z // 2), Z // 2)].reshape(D // 2, QC)
        g = (nn(w, g2[:, rows]) * s1[feats, rows].astype(F32)).astype(BF16)
        dT[feats, :] += nn(g, ob[p])
        return 0

    grad2(0)
    lax.fori_loop(0, 2, back, 0)
    grad2(1)
    grad2(2)
    grad2(3)

    def middle(i, _):
        one = at(K + i)
        two = at(K - 1 - i)
        at_one = pl.ds(pl.multiple_of(one * BK, BK), BK)
        at_two = pl.ds(pl.multiple_of(two * BK, BK), BK)
        both = nt(jnp.concatenate([h1[at_one, :], h1[at_two, :]], axis=0), g2[...])
        dW[one] = both[0:BK].reshape(Q, BK // Q, QC)
        dW[two] = both[BK:].reshape(Q, BK // Q, QC)
        return 0

    def rs_copy(way, k, p):
        return copy(
            rss.at[way, k - 1, p], rsb.at[way, k - 1, p], rs_s.at[way, k - 1, p], rs_r.at[way, k - 1, p], side[way]
        )

    def rs_in(way, k, p):
        copy(rsb.at[way, k, p], rsb.at[way, k, p], rs_s.at[way, k, p], rs_r.at[way, k, p], side[way]).wait_recv()
        return rsb[way, k, p].astype(F32)

    def rs_put(way, k, p, joined):
        v = dW[at(k if way == RIGHT else -k), p]
        if joined:
            v = v + rs_in(way, k, p)
        rss[way, k - 1, p] = v.astype(BF16)
        rs_copy(way, k, p).start()

    def rs_open(j, _):
        rs_put(RIGHT, K, j, False)
        rs_put(LEFT, K, 2 + j, False)
        return 0

    def rs_open2(j, _):
        rs_put(RIGHT, K - 1, 2 + j, False)
        rs_put(LEFT, K - 1, j, False)
        return 0

    def middle_open(i, _):
        middle(i, 0)

        @pl.when(i == 0)
        def _():
            lax.fori_loop(0, 2, rs_open, 0)

        return 0

    lax.fori_loop(0, 2, middle_open, 0)
    lax.fori_loop(0, 2, rs_open2, 0)

    acc = jnp.zeros((32, QC), F32)
    fit = jnp.zeros((1, ROWS), F32)
    for p in range(Q):
        acc = acc + nt(gr[p], h2[:, p * ROWS : (p + 1) * ROWS])
        x = gr[p].astype(F32)
        fit = fit + x[ACT : ACT + 1, :] + x[ACT + 1 : ACT + 2, :]
    at_head = lax.broadcasted_iota(jnp.int32, (24, QC), 0)
    fit_high = fit.astype(BF16).astype(F32)
    packed = jnp.where(at_head == ACT, fit_high, jnp.where(at_head == ACT + 1, fit - fit_high, acc[0:24, :]))
    dH[z] = packed.astype(BF16)

    def dh_out(off):
        i = NEAR.index(off)
        return copy(dH.at[z], dH.at[z], dh_s.at[i], dh_r.at[i], column(off))

    def dh_on(step, off):
        i = NEAR.index(off)
        ref = dH.at[at(-2 * step)]
        return copy(ref, ref, dh_s.at[i], dh_r.at[i], column(off - 2 * step))

    def dh_in(off):
        i = NEAR.index(off)
        ref = dH.at[at(-off)]
        copy(ref, ref, dh_s.at[i], dh_r.at[i], sib).wait_recv()

    for off in (2, -2, 1, -1):
        dh_out(off).start()

    def join3(j, _):
        rs_put(RIGHT, K - 1, j, True)
        rs_put(LEFT, K - 1, 2 + j, True)
        return 0

    def join2(j, _):
        rs_put(RIGHT, 2, lax.rem(2 + j, Q), True)
        rs_put(LEFT, 2, j, True)
        return 0

    lax.fori_loop(2, 4, back, 0)
    lax.fori_loop(0, 2, join3, 0)
    lax.fori_loop(2, 3, middle, 0)
    lax.fori_loop(0, 2, join2, 0)
    lax.fori_loop(4, 7, back, 0)
    lax.fori_loop(2, 4, join2, 0)
    lax.fori_loop(7, 8, back, 0)

    def turn_back(i, _):
        feats = pl.ds(pl.multiple_of(i * 256, 256), 256)
        x = 0.5 * jnp.transpose(dT[feats, :])
        dI[:, :, :, :, feats] = x.reshape(Z, 2, 2, 8, 256)
        return 0

    dh_in(2)
    dh_on(1, 3).start()
    dh_on(1, K).start()
    dh_in(-2)
    dh_on(-1, -3).start()
    lax.fori_loop(0, Z, turn_back, 0)

    for b in range(Z):
        for j in range(2):
            sib_s[b, j] = dI[b, j, 1 - c].astype(BF16)
    core_sum = copy(sib_s, sib_r, sb_s.at[8], sb_r.at[8], sib)
    core_sum.start()
    lax.fori_loop(3, 4, middle, 0)
    core_sum.wait_recv()

    def own_in(off, j):
        b = at(off)
        return dI[b, j, c] + sib_r[b, j].astype(F32)

    def ri_copy(way, k, j):
        return copy(
            ris.at[way, k - 1, j], rib.at[way, k - 1, j], ri_s.at[way, k - 1, j], ri_r.at[way, k - 1, j], side[way]
        )

    def ri_in(way, k, j):
        copy(rib.at[way, k, j], rib.at[way, k, j], ri_s.at[way, k, j], ri_r.at[way, k, j], side[way]).wait_recv()
        return rib[way, k, j].astype(F32)

    def ri_put(way, k, j, joined):
        v = own_in(k if way == RIGHT else -k, j)
        if joined:
            v = v + ri_in(way, k, j)
        ris[way, k - 1, j] = v.astype(BF16)
        ri_copy(way, k, j).start()

    ri_put(RIGHT, 4, 0, False)
    ri_put(LEFT, 4, 1, False)
    ri_put(RIGHT, 3, 1, False)
    ri_put(LEFT, 3, 0, False)

    lr = lrate[m]
    lr_before = lrate[m_before]
    rate = jnp.exp(jnp.full((8, 128), lr, F32))[0:1, 0:1]
    rate_before = jnp.exp(jnp.full((8, 128), lr_before, F32))[0:1, 0:1]
    flag = copyf[m]

    def next_out(p):
        return copy(nm.at[p], ym.at[q], y_s.at[p], y_r.at[q], {"pop": m_after, "dp": z * Q + p})

    def out_mate(p):
        return copy(nm.at[p], om.at[q], gp_s.at[OUT, p], gp_r.at[OUT, q], {"dp": z * Q + p})

    def middle_end(p):
        g = dW[z, p] + rs_in(RIGHT, 0, p) + rs_in(LEFT, 0, p)
        nm[p] = (wq[z, p].astype(F32) - rate * g).astype(BF16)
        next_out(p).start()

        @pl.when(p != q)
        def _():
            out_mate(p).start()

    def ones(j, _):
        rs_put(RIGHT, 1, lax.rem(2 + j, Q), True)
        rs_put(LEFT, 1, j, True)
        return 0

    lax.fori_loop(0, 2, ones, 0)
    ri_put(RIGHT, 3, 0, True)
    ri_put(LEFT, 3, 1, True)
    lax.fori_loop(2, 4, ones, 0)
    for j in range(2):
        ri_put(RIGHT, 2, j, True)
        ri_put(LEFT, 2, j, True)
    for off in (1, -1, 3, -3, K):
        dh_in(off)
    tot = dH[0].astype(F32)
    for b in range(1, Z):
        tot = tot + dH[b].astype(F32)
    dHg[q] = tot
    o_fit[0] = jnp.sum(tot[ACT : ACT + 2, :])

    def dh_mate(t):
        return copy(dHg.at[q], dHg.at[q], gp_s.at[DH, mate(t)], gp_r.at[DH, q], mate_id(t))

    for t in (2, 1, 3):
        dh_mate(t).start()

    middle_end(0)
    middle_end(2)
    middle_end(1)
    middle_end(3)
    for j in range(2):
        ri_put(RIGHT, 1, j, True)
        ri_put(LEFT, 1, j, True)
    for t in (2, 1, 3):
        p = mate(t)
        copy(dHg.at[p], dHg.at[p], gp_s.at[DH, p], gp_r.at[DH, p], sib).wait_recv()
    tH[...] = jnp.transpose(dHg[z // 2])
    own_rows = pl.ds(pl.multiple_of(lax.rem(d, Z) * 64, 64), 64)
    nh[...] = (wh[z, h, c].astype(F32) - rate * jnp.transpose(tH[own_rows, :])[0:ACT, :]).astype(BF16)
    head_y = copy(nh, yh, y_s.at[5], y_r.at[5], after)
    head_y.start()
    for j in range(2):
        tin[j] = own_in(0, j) + ri_in(RIGHT, 0, j) + ri_in(LEFT, 0, j)
    xs[...] = tin[1 - h].astype(BF16)
    cross = copy(xs, xr, xp_s.at[2], xp_r.at[2], xpt)
    cross.start()
    cross_y = copy(xs, xp, xp_s.at[0], xp_r.at[0], {"pop": m_after, "dp": xpt["dp"]})
    cross_y.start()
    ni[...] = tin[h].astype(BF16)
    in_y = copy(ni, yi, y_s.at[4], y_r.at[4], after)
    in_y.start()
    def chosen(got, own):
        return jnp.where(jnp.full(own.shape, flag) == 1, got.astype(F32), own.astype(F32)).astype(BF16)

    for t in (0, 1, 2, 3):
        p = mate(t)
        own = nm.at[p] if t == 0 else om.at[p]
        if t:
            copy(own, own, gp_s.at[OUT, p], gp_r.at[OUT, p], sib).wait_recv()
        copy(ym.at[p], ym.at[p], y_s.at[p], y_r.at[p], after).wait_recv()
        o_mid[:, pl.ds(pl.multiple_of(p * QC, QC), QC)] = chosen(ym[p], own[...])
    pick = pert[m]
    o_rate[0] = jnp.where(flag == 1, lr_before, lr) + jnp.where(pick == 0, -0.2, jnp.where(pick == 1, 0.0, 0.2))
    head_y.wait_recv()
    o_head[...] = chosen(yh[...], nh[...])
    prior.wait_recv()
    cross.wait_recv()
    cross_y.wait_recv()
    in_y.wait_recv()
    new = wi[z, h, c].astype(F32) - rate * (tin[h] + xr[...].astype(F32))
    new_before = wp[...].astype(F32) - rate_before * (yi[...].astype(F32) + xp[...].astype(F32))
    o_in[...] = chosen(new_before, new)

    for off in NEAR:
        if off in (1, -1, 2, -2):
            win_out(off).wait_send()
        else:
            win_on(1 if off > 0 else -1, off).wait_send()
        win_x(off).wait_send()
    win_x(0).wait_send()
    prior.wait_send()
    cross_y.wait_send()
    for p in range(Q):
        next_out(p).wait_send()
    xwh.wait_send()
    cross.wait_send()
    head_y.wait_send()
    in_y.wait_send()
    for i in range(8):
        core_copy(core_off[i], i).wait_send()
    head_core.wait_send()
    sight_x.wait_send()
    sight_core.wait_send()
    sight_on.wait_send()
    core_sum.wait_send()
    for t in (1, 2, 3):
        quarter(t).wait_send()
        raw_out(mate(t)).wait_send()
        gr_out(t).wait_send()
        dh_mate(t).wait_send()
        out_mate(mate(t)).wait_send()
    for k in range(1, K):
        for way in (RIGHT, LEFT):
            for j in range(2):
                for kind in MID:
                    ag(kind, way, k, j).wait_send()
                ri_copy(way, k, j).wait_send()
            for p in range(Q):
                rs_copy(way, k, p).wait_send()
    for kind in MID:
        ag(kind, RIGHT, K, 0).wait_send()
        ag(kind, LEFT, K, 1).wait_send()
    ri_copy(RIGHT, K, 0).wait_send()
    ri_copy(LEFT, K, 1).wait_send()
    for j in range(2):
        rs_copy(RIGHT, K, j).wait_send()
        rs_copy(LEFT, K, 2 + j).wait_send()
    for off in (1, -1, 2, -2):
        dh_out(off).wait_send()
    for off in (3, -3, K):
        dh_on(1 if off > 0 else -1, off).wait_send()


def local(observations, returns, actions, w_input, w_middle, w_head, log_rate, copy_from, perturb):
    hbm = pl.BlockSpec(memory_space=pltpu.HBM)
    vmem = pl.BlockSpec(memory_space=pltpu.VMEM)
    smem = pl.BlockSpec(memory_space=pltpu.SMEM)
    V = pltpu.VMEM
    S = pltpu.SemaphoreType.DMA
    out = pl.pallas_call(
        kernel,
        out_shape=(
            pltpu.VMEM((8, D), BF16),
            pltpu.VMEM((64, D), BF16),
            pltpu.VMEM((ACT, 64), BF16),
            jax.ShapeDtypeStruct((1,), F32),
            jax.ShapeDtypeStruct((1,), F32),
        ),
        in_specs=[hbm, vmem, vmem, hbm, hbm, hbm, smem, smem, smem],
        out_specs=(vmem, vmem, vmem, smem, smem),
        scratch_shapes=[
            V((Q, ROWS, OBS), BF16),
            V((OBS, D), BF16),
            V((Z, 2, 2, 8, D), BF16),
            V((Z, 2, 2, ACT, 64), BF16),
            V((Z, Q, 64, QC), BF16),
            V((D, OBS), BF16),
            V((2, QC, BK), BF16),
            V((D, OBS), F32),
            V((D, D), BF16),
            V((D, D), BF16),
            V((QC, D), F32),
            V((QC, D), BF16),
            V((QC, D), BF16),
            V((128, QC), F32),
            V((QC, 128), BF16),
            V((32, QC), BF16),
            V((Q, 24, ROWS), F32),
            V((Q, 24, ROWS), F32),
            V((Q, 32, ROWS), BF16),
            V((Z, Q, 64, QC), F32),
            V((2, K, Q, 64, QC), BF16),
            V((2, K, Q, 64, QC), BF16),
            V((Z, 2, 2, 8, D), F32),
            V((Z, 2, 8, D), BF16),
            V((Z, 2, 8, D), BF16),
            V((2, K, 2, 8, D), BF16),
            V((2, K, 2, 8, D), BF16),
            V((2, 8, D), F32),
            V((8, D), BF16),
            V((8, D), BF16),
            V((8, D), BF16),
            V((8, D), BF16),
            V((Z, 24, QC), BF16),
            V((Q, 24, QC), F32),
            V((QC, 24), F32),
            V((Q, 64, QC), BF16),
            V((Q, 64, QC), BF16),
            V((Q, 64, QC), BF16),
            V((8, D), BF16),
            V((8, D), BF16),
            V((ACT, 64), BF16),
            V((ACT, 64), BF16),
            S((2, 2, K, 2)), S((2, 2, K, 2)),
            S((7,)), S((7,)),
            S((8,)), S((8,)),
            S((6, Q)), S((6, Q)),
            S((3,)), S((3,)),
            S((10,)), S((10,)),
            S((7,)), S((7,)),
            S((2, K, Q)), S((2, K, Q)),
            S((2, K, 2)), S((2, K, 2)),
            S((7,)), S((7,)),
            S((4,)),
        ],
        compiler_params=pltpu.CompilerParams(
            collective_id=0, has_side_effects=True, vmem_limit_bytes=60 * 1024 * 1024
        ),
    )(observations[0], returns, actions, w_input[0], w_middle[0], w_head[0].T, log_rate, copy_from, perturb)
    return out[0][None], out[1][None], out[2].T[None], out[3], out[4]


def solution(mesh):
    in_specs = (
        P("pop", "dp", None),
        P("pop", "dp"),
        P("pop", "dp"),
        P("pop", "dp", None),
        P("pop", "dp", None),
        P("pop", "dp", None),
        P(),
        P(),
        P(),
    )
    out_specs = (
        P("pop", "dp", None),
        P("pop", "dp", None),
        P("pop", "dp", None),
        P("pop"),
        P("pop"),
    )
    return jax.shard_map(local, mesh=mesh, in_specs=in_specs, out_specs=out_specs, check_vma=False)
```

```python
import jax
import jax.numpy as jnp
from jax import lax
from jax.experimental import pallas as pl
from jax.experimental.pallas import tpu as pltpu
from jax.sharding import PartitionSpec as P

F32 = jnp.float32
BF16 = jnp.bfloat16
Z = 8
K = Z // 2
Q = 4
ROWS = 512
OBS = 256
D = 2048
QC = D // Q
BK = D // Z
ACT = 18
POP = 8
BATCH = ROWS * Z * Q
WM, WH = 0, 1
OB, QT, RAW, GR, DH, OUT = range(6)
RIGHT, LEFT = 0, 1
NEAR = (1, -1, 2, -2, 3, -3, K)


def nt(a, b):
    return lax.dot_general(a, b, (((1,), (1,)), ((), ())), preferred_element_type=F32)


def nn(a, b):
    return jnp.dot(a, b, preferred_element_type=F32)


def kernel(
    obs, ret, act, win, wmid, whead, lrate, copyf, pert,
    o_in, o_mid, o_head, o_rate, o_fit,
    ob, obT, wi, wh, wq, w1T, wT, dT, h1, s1, p2, h2, g2, whp, whq, whT,
    raw_s, raw_r, gr, dW, rss, rsb, dI, sib_s, sib_r, ris, rib, tin, xs, xr,
    xp, wp, dH, dHg, tH, nm, ym, om, ni, yi, nh, yh,
    ag_s, ag_r, wz_s, wz_r, wx_s, wx_r, gp_s, gp_r, xp_s, xp_r, sb_s, sb_r, dh_s, dh_r, rs_s, rs_r, ri_s, ri_r, y_s, y_r, loc,
):
    m = lax.axis_index("pop")
    d = lax.axis_index("dp")
    z = d // Q
    q = lax.rem(d, Q)
    h = q // 2
    c = lax.rem(q, 2)
    sib = {"dp": z * Q + h * 2 + (1 - c)}
    xpt = {"dp": z * Q + (1 - h) * 2 + c}
    side = [{"dp": lax.rem(z + 1, Z) * Q + q}, {"dp": lax.rem(z + Z - 1, Z) * Q + q}]
    after = {"pop": lax.rem(m + 1, POP)}
    m_after = lax.rem(m + 1, POP)
    m_before = lax.rem(m + POP - 1, POP)
    before = {"pop": m_before}

    def mate(t):
        return lax.rem(q + t, Q)

    def mate_id(t):
        return {"dp": z * Q + mate(t)}

    def at(off):
        return lax.rem(z + off + Z, Z)

    def column(off):
        return {"dp": at(off) * Q + q}

    def copy(src, dst, ss, rs, dev):
        return pltpu.make_async_remote_copy(
            src_ref=src, dst_ref=dst, send_sem=ss, recv_sem=rs, device_id=dev,
            device_id_type=pl.DeviceIdType.MESH,
        )

    fetch = [
        pltpu.make_async_copy(win, wi.at[z, h, c], loc.at[0]),
        pltpu.make_async_copy(wmid.at[:, pl.ds(pl.multiple_of(q * QC, QC), QC)], wq.at[z, q], loc.at[1]),
        pltpu.make_async_copy(whead, wh.at[z, h, c], loc.at[2]),
        pltpu.make_async_copy(obs, ob.at[q], loc.at[3]),
    ]
    for f in fetch:
        f.start()

    barrier = pltpu.get_barrier_semaphore()
    met = [mate_id(t) for t in (1, 2, 3)] + [after, before] + [column(off) for off in (2, -2, 1, -1)]
    for near in (m_after, m_before):
        met += [{"pop": near, "dp": z * Q + mate(t)} for t in (1, 2, 3)]
    for dev in met:
        pl.semaphore_signal(barrier, inc=1, device_id=dev, device_id_type=pl.DeviceIdType.MESH)
    pl.semaphore_wait(barrier, len(met))

    def win_out(off):
        i = NEAR.index(off)
        return copy(win, wi.at[z, h, c], wz_s.at[i], wz_r.at[i], column(off))

    def win_in(off):
        i = NEAR.index(off)
        ref = wi.at[at(-off), h, c]
        copy(ref, ref, wz_s.at[i], wz_r.at[i], xpt).wait_recv()

    def win_x(off):
        i = 7 if off == 0 else NEAR.index(off)
        ref = wi.at[at(-off), h, c]
        return copy(win if off == 0 else ref, ref, wx_s.at[i], wx_r.at[i], xpt)

    def win_x_in(off):
        i = 7 if off == 0 else NEAR.index(off)
        ref = wi.at[at(-off), 1 - h, c]
        copy(ref, ref, wx_s.at[i], wx_r.at[i], xpt).wait_recv()

    def win_on(step, off):
        i = NEAR.index(off)
        ref = wi.at[at(-2 * step), h, c]
        return copy(ref, ref, wz_s.at[i], wz_r.at[i], column(off - 2 * step))

    for off in (2, -2, 1, -1):
        win_out(off).start()
    win_x(0).start()
    prior = copy(win, wp, y_s.at[6], y_r.at[6], after)
    xwh = copy(whead, wh.at[z, h, c], xp_s.at[1], xp_r.at[1], xpt)

    def quarter(t):
        p = mate(t)
        return copy(
            wmid.at[:, pl.ds(pl.multiple_of(p * QC, QC), QC)], wq.at[z, q], gp_s.at[QT, p], gp_r.at[QT, q], mate_id(t)
        )

    x_mate = (1 - h) * 2 + c
    sight_x = copy(obs, ob.at[q], gp_s.at[OB, 0], gp_r.at[OB, q], xpt)
    sight_core = copy(obs, ob.at[q], gp_s.at[OB, 1], gp_r.at[OB, q], sib)
    sight_on = copy(ob.at[x_mate], ob.at[x_mate], gp_s.at[OB, 2], gp_r.at[OB, x_mate], sib)

    def quarter_in(p):
        copy(wq.at[z, p], wq.at[z, p], gp_s.at[QT, p], gp_r.at[QT, p], sib).wait_recv()

    for t in (1, 2, 3):
        quarter(t).start()
    xwh.start()
    sight_core.start()
    prior.start()
    p2[...] = jnp.zeros_like(p2)
    dT[...] = jnp.zeros_like(dT)

    def piece(kind, b, j):
        if kind == WM:
            return wq.at[b, pl.ds(2 * j, 2)]
        return wh.at[b, j, c]

    def ag(kind, way, k, j):
        b = at(1 - k) if way == RIGHT else at(k - 1)
        ref = piece(kind, b, j)
        return copy(ref, ref, ag_s.at[kind, way, k - 1, j], ag_r.at[kind, way, k - 1, j], side[way])

    def ag_in(kind, way, k, j):
        b = at(-k) if way == RIGHT else at(k)
        ref = piece(kind, b, j)
        copy(ref, ref, ag_s.at[kind, way, k - 1, j], ag_r.at[kind, way, k - 1, j], side[way]).wait_recv()

    def put(kinds, k, j):
        for kind in kinds:
            for way in (RIGHT, LEFT):
                ag(kind, way, k, j).start()

    def take(kinds, k, j):
        for kind in kinds:
            for way in (RIGHT, LEFT):
                ag_in(kind, way, k, j)

    def take_last(kinds, k):
        for kind in kinds:
            ag_in(kind, RIGHT, k, 0)
            ag_in(kind, LEFT, k, 1)

    def put_last(kinds):
        for kind in kinds:
            ag(kind, RIGHT, K, 0).start()
            ag(kind, LEFT, K, 1).start()

    MID = (WM, WH)

    def core_copy(off, i):
        b = at(-off)
        return copy(wi.at[b, :, c], wi.at[b, :, c], sb_s.at[i], sb_r.at[i], sib)

    def core_in(off, i):
        b = at(-off)
        copy(wi.at[b, :, 1 - c], wi.at[b, :, 1 - c], sb_s.at[i], sb_r.at[i], sib).wait_recv()

    core_off = (0,) + NEAR
    head_core = copy(wh.at[:, :, c], wh.at[:, :, c], sb_s.at[9], sb_r.at[9], sib)

    def head_core_in():
        copy(wh.at[:, :, 1 - c], wh.at[:, :, 1 - c], sb_s.at[9], sb_r.at[9], sib).wait_recv()

    def obs_in(p):
        copy(ob.at[p], ob.at[p], gp_s.at[OB, 0], gp_r.at[OB, p], sib).wait_recv()

    def group_at(i):
        return (h + i // 2 * (1 - 2 * h)) * 2 + c + i % 2 * (1 - 2 * c)

    def turn_by(i, _):
        p = group_at(i)
        cols = pl.ds(pl.multiple_of(p * ROWS, ROWS), ROWS)
        obT[:, cols] = jnp.transpose(ob[p].astype(F32)).astype(BF16)
        return 0

    for off in NEAR[:2]:
        win_in(off)
        win_x(off).start()
    for off in NEAR[2:4]:
        win_in(off)
        win_on(off // 2, 3 * off // 2).start()
        if off > 0:
            win_on(1, K).start()
        win_x(off).start()
    fetch[1].wait()
    fetch[2].wait()
    quarter_in(h * 2 + (1 - c))
    put(MID, 1, h)
    quarter_in((1 - h) * 2)
    quarter_in((1 - h) * 2 + 1)
    xwh.wait_recv()
    put(MID, 1, 1 - h)
    fetch[3].wait()
    turn_by(0, 0)
    obs_in(h * 2 + (1 - c))
    turn_by(1, 0)
    for off in NEAR[4:]:
        win_in(off)
        win_x(off).start()
    sight_x.start()
    fetch[0].wait()
    for i, off in enumerate(core_off[:5]):
        win_x_in(off)
        core_copy(off, i).start()
    take(MID, 1, h)
    put(MID, 2, h)
    for i, off in enumerate(core_off[5:]):
        win_x_in(off)
        core_copy(off, 5 + i).start()
    take(MID, 1, 1 - h)
    put(MID, 2, 1 - h)
    for i in range(8):
        core_in(core_off[i], i)

    def turn_in(i, _):
        cols = pl.ds(pl.multiple_of(i * 256, 256), 256)
        x = wi[:, :, :, :, cols].astype(F32).reshape(OBS, 256)
        w1T[cols, :] = (0.5 * jnp.transpose(x)).astype(BF16)
        return 0

    lax.fori_loop(0, D // 256, turn_in, 0)

    def block_of(i):
        return at(((i + 1) // 2) * (2 * lax.rem(i + 1, 2) - 1))

    def first(i, p):
        feats = pl.ds(pl.multiple_of(i * BK, BK), BK)
        rows = pl.ds(pl.multiple_of(p * ROWS, ROWS), ROWS)
        u = nn(w1T[feats, :], obT[:, rows])
        t = jnp.tanh(u)
        a = 1.0 + t
        hid = u * a
        h1[feats, rows] = hid.astype(BF16)
        s1[feats, rows] = (a + hid * (1.0 - t)).astype(BF16)

    def block_rows(i):
        return pl.ds(pl.multiple_of(block_of(i) * BK, BK), BK)

    def turn_w(i):
        for b in range(2):
            x = wq[block_of(2 * i + b)].astype(F32).reshape(BK, QC)
            wT[b] = (0.5 * jnp.transpose(x)).astype(BF16)

    def second(i, rows):
        p2[:, rows] += nn(wT[0], h1[block_rows(2 * i), rows]) + nn(wT[1], h1[block_rows(2 * i + 1), rows])

    def first_by(i, _):
        @pl.when(i == 1)
        def _():
            with jax.named_scope("wait1"):
                take(MID, 2, h)
                put(MID, 3, h)

        @pl.when(i == 3)
        def _():
            with jax.named_scope("wait3"):
                obs_in(x_mate)
                sight_on.start()
                turn_by(2, 0)

        @pl.when(i == 4)
        def _():
            with jax.named_scope("wait4"):
                take(MID, 2, 1 - h)
                put(MID, 3, 1 - h)
                obs_in((1 - h) * 2 + (1 - c))
                turn_by(3, 0)

        @pl.when(i == 6)
        def _():
            with jax.named_scope("wait6"):
                take_last(MID, 3)
                put_last(MID)

        for b in range(2):
            for p in range(2):
                first(i % K * 2 + b, group_at(i // K * 2 + p))
        return 0

    def second_by(i, _):
        @pl.when(i == 2)
        def _():
            with jax.named_scope("wait2s"):
                for kind in MID:
                    ag_in(kind, RIGHT, 3, 1)
                    ag_in(kind, LEFT, 3, 0)
                take_last(MID, K)
                head_core.start()

        turn_w(i)
        for p in range(Q):
            second(i, slice(p * ROWS, (p + 1) * ROWS))
        return 0

    lax.fori_loop(0, Z, first_by, 0)
    lax.fori_loop(0, K - 1, second_by, 0)
    turn_w(K - 1)

    head_core_in()
    whp[...] = jnp.zeros_like(whp)
    for b in range(2):
        for i in range(Q):
            lanes = slice((b * Q + i) * 64, (b * Q + i + 1) * 64)
            whp[0:ACT, lanes] = wh[2 * q + b, i // 2, i % 2].astype(F32)
    whT[...] = whp[0:32, :].astype(BF16)
    whq[...] = jnp.transpose(whp[...]).astype(BF16)

    def raw_out(p):
        return copy(raw_s.at[p], raw_r.at[q], gp_s.at[RAW, p], gp_r.at[RAW, q], {"dp": z * Q + p})

    for t in (2, 1, 3, 0):
        p = mate(t)
        rows = pl.ds(pl.multiple_of(p * ROWS, ROWS), ROWS)

        second(K - 1, rows)

        def forward2(i, _):
            cols = pl.ds(pl.multiple_of(p * ROWS + i * 128, 128), 128)
            u = p2[:, cols]
            h2[:, cols] = (u + u * jnp.tanh(u)).astype(BF16)
            return 0

        lax.fori_loop(0, 4, forward2, 0)
        raw_s[p] = nn(whT[...], h2[:, rows])[0:24, :]
        if t:
            raw_out(p).start()
    def slope2(i, _):
        cols = pl.ds(pl.multiple_of(i * 128, 128), 128)
        u = p2[:, cols]
        t = jnp.tanh(u)
        a = 1.0 + t
        p2[:, cols] = a + u * a * (1.0 - t)
        return 0

    lax.fori_loop(0, D // 128, slope2, 0)
    raw = raw_s[q]
    for t in (2, 1, 3):
        p = mate(t)
        copy(raw_r.at[p], raw_r.at[p], gp_s.at[RAW, p], gp_r.at[RAW, p], sib).wait_recv()
        raw = raw + raw_r[p]
    at_act = lax.broadcasted_iota(jnp.int32, raw.shape, 0)
    squash = jnp.tanh(raw * 0.5)
    logits = 2.0 * squash
    e = jnp.where(at_act < ACT, jnp.exp(logits), 0.0)
    total = jnp.sum(e, axis=0, keepdims=True)
    logp = logits - jnp.log(total)
    onehot = jnp.where(at_act == act[...], 1.0, 0.0)
    gains = ret[...] * (1.0 / BATCH)
    term = gains * jnp.sum(logp * onehot, axis=0, keepdims=True)
    grad = -gains * (onehot - e / total) * (1.0 - squash * squash)
    high = term.astype(BF16).astype(F32)
    low = term - high
    grad = jnp.where(at_act < ACT, grad, jnp.where(at_act == ACT, high, jnp.where(at_act == ACT + 1, low, 0.0)))
    gr[q] = jnp.concatenate([grad, jnp.zeros((8, ROWS), F32)], axis=0).astype(BF16)

    def gr_out(t):
        return copy(gr.at[q], gr.at[q], gp_s.at[GR, mate(t)], gp_r.at[GR, q], mate_id(t))

    for t in (2, 1, 3):
        gr_out(t).start()
    wb = (0.5 * whq[:, 0:32].astype(F32)).astype(BF16)

    def grad2(i):
        p = group_at(i)
        if i:
            copy(gr.at[p], gr.at[p], gp_s.at[GR, p], gp_r.at[GR, p], sib).wait_recv()
        rows = pl.ds(pl.multiple_of(p * ROWS, ROWS), ROWS)
        g2[:, rows] = (nn(wb, gr[p]) * p2[:, rows]).astype(BF16)

    def back(i, _):
        p = group_at(i // 2)
        rows = pl.ds(pl.multiple_of(p * ROWS, ROWS), ROWS)
        half = lax.rem(i, 2)
        feats = pl.ds(pl.multiple_of(half * (D // 2), D // 2), D // 2)
        w = wq[pl.ds(half * (Z // 2), Z // 2)].reshape(D // 2, QC)
        g = (nn(w, g2[:, rows]) * s1[feats, rows].astype(F32)).astype(BF16)
        dT[feats, :] += nn(g, ob[p])
        return 0

    grad2(0)
    lax.fori_loop(0, 2, back, 0)
    grad2(1)
    grad2(2)
    grad2(3)

    def middle(i, _):
        one = at(K + i)
        two = at(K - 1 - i)
        at_one = pl.ds(pl.multiple_of(one * BK, BK), BK)
        at_two = pl.ds(pl.multiple_of(two * BK, BK), BK)
        both = nt(jnp.concatenate([h1[at_one, :], h1[at_two, :]], axis=0), g2[...])
        dW[one] = both[0:BK].reshape(Q, BK // Q, QC)
        dW[two] = both[BK:].reshape(Q, BK // Q, QC)
        return 0

    def rs_copy(way, k, p):
        return copy(
            rss.at[way, k - 1, p], rsb.at[way, k - 1, p], rs_s.at[way, k - 1, p], rs_r.at[way, k - 1, p], side[way]
        )

    def rs_in(way, k, p):
        copy(rsb.at[way, k, p], rsb.at[way, k, p], rs_s.at[way, k, p], rs_r.at[way, k, p], side[way]).wait_recv()
        return rsb[way, k, p].astype(F32)

    def rs_put(way, k, p, joined):
        v = dW[at(k if way == RIGHT else -k), p]
        if joined:
            v = v + rs_in(way, k, p)
        rss[way, k - 1, p] = v.astype(BF16)
        rs_copy(way, k, p).start()

    def rs_open(j, _):
        rs_put(RIGHT, K, j, False)
        rs_put(LEFT, K, 2 + j, False)
        return 0

    def rs_open2(j, _):
        rs_put(RIGHT, K - 1, 2 + j, False)
        rs_put(LEFT, K - 1, j, False)
        return 0

    def middle_open(i, _):
        middle(i, 0)

        @pl.when(i == 0)
        def _():
            lax.fori_loop(0, 2, rs_open, 0)

        return 0

    lax.fori_loop(0, 2, middle_open, 0)
    lax.fori_loop(0, 2, rs_open2, 0)

    acc = jnp.zeros((32, QC), F32)
    fit = jnp.zeros((1, ROWS), F32)
    for p in range(Q):
        acc = acc + nt(gr[p], h2[:, p * ROWS : (p + 1) * ROWS])
        x = gr[p].astype(F32)
        fit = fit + x[ACT : ACT + 1, :] + x[ACT + 1 : ACT + 2, :]
    at_head = lax.broadcasted_iota(jnp.int32, (24, QC), 0)
    fit_high = fit.astype(BF16).astype(F32)
    packed = jnp.where(at_head == ACT, fit_high, jnp.where(at_head == ACT + 1, fit - fit_high, acc[0:24, :]))
    dH[z] = packed.astype(BF16)

    def dh_out(off):
        i = NEAR.index(off)
        return copy(dH.at[z], dH.at[z], dh_s.at[i], dh_r.at[i], column(off))

    def dh_on(step, off):
        i = NEAR.index(off)
        ref = dH.at[at(-2 * step)]
        return copy(ref, ref, dh_s.at[i], dh_r.at[i], column(off - 2 * step))

    def dh_in(off):
        i = NEAR.index(off)
        ref = dH.at[at(-off)]
        copy(ref, ref, dh_s.at[i], dh_r.at[i], sib).wait_recv()

    for off in (2, -2, 1, -1):
        dh_out(off).start()

    def join3(j, _):
        rs_put(RIGHT, K - 1, j, True)
        rs_put(LEFT, K - 1, 2 + j, True)
        return 0

    def join2(j, _):
        rs_put(RIGHT, 2, lax.rem(2 + j, Q), True)
        rs_put(LEFT, 2, j, True)
        return 0

    lax.fori_loop(2, 5, back, 0)
    lax.fori_loop(0, 2, join3, 0)
    lax.fori_loop(2, 3, middle, 0)
    lax.fori_loop(5, 6, back, 0)
    lax.fori_loop(0, 2, join2, 0)
    lax.fori_loop(6, 8, back, 0)
    def turn_back(i, _):
        feats = pl.ds(pl.multiple_of(i * 256, 256), 256)
        x = 0.5 * jnp.transpose(dT[feats, :])
        dI[:, :, :, :, feats] = x.reshape(Z, 2, 2, 8, 256)
        return 0

    dh_in(2)
    dh_on(1, 3).start()
    dh_on(1, K).start()
    dh_in(-2)
    dh_on(-1, -3).start()
    lax.fori_loop(0, Z, turn_back, 0)

    for b in range(Z):
        for j in range(2):
            sib_s[b, j] = dI[b, j, 1 - c].astype(BF16)
    core_sum = copy(sib_s, sib_r, sb_s.at[8], sb_r.at[8], sib)
    core_sum.start()
    lax.fori_loop(2, 4, join2, 0)
    lax.fori_loop(3, 4, middle, 0)
    core_sum.wait_recv()

    def own_in(off, j):
        b = at(off)
        return dI[b, j, c] + sib_r[b, j].astype(F32)

    def ri_copy(way, k, j):
        return copy(
            ris.at[way, k - 1, j], rib.at[way, k - 1, j], ri_s.at[way, k - 1, j], ri_r.at[way, k - 1, j], side[way]
        )

    def ri_in(way, k, j):
        copy(rib.at[way, k, j], rib.at[way, k, j], ri_s.at[way, k, j], ri_r.at[way, k, j], side[way]).wait_recv()
        return rib[way, k, j].astype(F32)

    def ri_put(way, k, j, joined):
        v = own_in(k if way == RIGHT else -k, j)
        if joined:
            v = v + ri_in(way, k, j)
        ris[way, k - 1, j] = v.astype(BF16)
        ri_copy(way, k, j).start()

    ri_put(RIGHT, 4, 0, False)
    ri_put(LEFT, 4, 1, False)
    ri_put(RIGHT, 3, 1, False)
    ri_put(LEFT, 3, 0, False)

    lr = lrate[m]
    lr_before = lrate[m_before]
    rate = jnp.exp(jnp.full((8, 128), lr, F32))[0:1, 0:1]
    rate_before = jnp.exp(jnp.full((8, 128), lr_before, F32))[0:1, 0:1]
    flag = copyf[m]

    def next_out(p):
        return copy(nm.at[p], ym.at[q], y_s.at[p], y_r.at[q], {"pop": m_after, "dp": z * Q + p})

    def out_mate(p):
        return copy(nm.at[p], om.at[q], gp_s.at[OUT, p], gp_r.at[OUT, q], {"dp": z * Q + p})

    def middle_end(p):
        g = dW[z, p] + rs_in(RIGHT, 0, p) + rs_in(LEFT, 0, p)
        nm[p] = (wq[z, p].astype(F32) - rate * g).astype(BF16)
        next_out(p).start()

        @pl.when(p != q)
        def _():
            out_mate(p).start()

    def ones(j, _):
        rs_put(RIGHT, 1, lax.rem(2 + j, Q), True)
        rs_put(LEFT, 1, j, True)
        return 0

    lax.fori_loop(0, 2, ones, 0)
    ri_put(RIGHT, 3, 0, True)
    ri_put(LEFT, 3, 1, True)
    lax.fori_loop(2, 4, ones, 0)
    for j in range(2):
        ri_put(RIGHT, 2, j, True)
        ri_put(LEFT, 2, j, True)
    for off in (1, -1, 3, -3, K):
        dh_in(off)
    tot = dH[0].astype(F32)
    for b in range(1, Z):
        tot = tot + dH[b].astype(F32)
    dHg[q] = tot
    o_fit[0] = jnp.sum(tot[ACT : ACT + 2, :])

    def dh_mate(t):
        return copy(dHg.at[q], dHg.at[q], gp_s.at[DH, mate(t)], gp_r.at[DH, q], mate_id(t))

    for t in (2, 1, 3):
        dh_mate(t).start()

    middle_end(0)
    middle_end(2)
    middle_end(1)
    middle_end(3)
    for j in range(2):
        ri_put(RIGHT, 1, j, True)
        ri_put(LEFT, 1, j, True)
    for t in (2, 1, 3):
        p = mate(t)
        copy(dHg.at[p], dHg.at[p], gp_s.at[DH, p], gp_r.at[DH, p], sib).wait_recv()
    tH[...] = jnp.transpose(dHg[z // 2])
    own_rows = pl.ds(pl.multiple_of(lax.rem(d, Z) * 64, 64), 64)
    nh[...] = (wh[z, h, c].astype(F32) - rate * jnp.transpose(tH[own_rows, :])[0:ACT, :]).astype(BF16)
    head_y = copy(nh, yh, y_s.at[5], y_r.at[5], after)
    head_y.start()
    for j in range(2):
        tin[j] = own_in(0, j) + ri_in(RIGHT, 0, j) + ri_in(LEFT, 0, j)
    xs[...] = tin[1 - h].astype(BF16)
    cross = copy(xs, xr, xp_s.at[2], xp_r.at[2], xpt)
    cross.start()
    cross_y = copy(xs, xp, xp_s.at[0], xp_r.at[0], {"pop": m_after, "dp": xpt["dp"]})
    cross_y.start()
    ni[...] = tin[h].astype(BF16)
    in_y = copy(ni, yi, y_s.at[4], y_r.at[4], after)
    in_y.start()
    def chosen(got, own):
        return jnp.where(jnp.full(own.shape, flag) == 1, got.astype(F32), own.astype(F32)).astype(BF16)

    for t in (0, 1, 2, 3):
        p = mate(t)
        own = nm.at[p] if t == 0 else om.at[p]
        if t:
            copy(own, own, gp_s.at[OUT, p], gp_r.at[OUT, p], sib).wait_recv()
        copy(ym.at[p], ym.at[p], y_s.at[p], y_r.at[p], after).wait_recv()
        o_mid[:, pl.ds(pl.multiple_of(p * QC, QC), QC)] = chosen(ym[p], own[...])
    pick = pert[m]
    o_rate[0] = jnp.where(flag == 1, lr_before, lr) + jnp.where(pick == 0, -0.2, jnp.where(pick == 1, 0.0, 0.2))
    head_y.wait_recv()
    o_head[...] = chosen(yh[...], nh[...])
    prior.wait_recv()
    cross.wait_recv()
    cross_y.wait_recv()
    in_y.wait_recv()
    new = wi[z, h, c].astype(F32) - rate * (tin[h] + xr[...].astype(F32))
    new_before = wp[...].astype(F32) - rate_before * (yi[...].astype(F32) + xp[...].astype(F32))
    o_in[...] = chosen(new_before, new)

    for off in NEAR:
        if off in (1, -1, 2, -2):
            win_out(off).wait_send()
        else:
            win_on(1 if off > 0 else -1, off).wait_send()
        win_x(off).wait_send()
    win_x(0).wait_send()
    prior.wait_send()
    cross_y.wait_send()
    for p in range(Q):
        next_out(p).wait_send()
    xwh.wait_send()
    cross.wait_send()
    head_y.wait_send()
    in_y.wait_send()
    for i in range(8):
        core_copy(core_off[i], i).wait_send()
    head_core.wait_send()
    sight_x.wait_send()
    sight_core.wait_send()
    sight_on.wait_send()
    core_sum.wait_send()
    for t in (1, 2, 3):
        quarter(t).wait_send()
        raw_out(mate(t)).wait_send()
        gr_out(t).wait_send()
        dh_mate(t).wait_send()
        out_mate(mate(t)).wait_send()
    for k in range(1, K):
        for way in (RIGHT, LEFT):
            for j in range(2):
                for kind in MID:
                    ag(kind, way, k, j).wait_send()
                ri_copy(way, k, j).wait_send()
            for p in range(Q):
                rs_copy(way, k, p).wait_send()
    for kind in MID:
        ag(kind, RIGHT, K, 0).wait_send()
        ag(kind, LEFT, K, 1).wait_send()
    ri_copy(RIGHT, K, 0).wait_send()
    ri_copy(LEFT, K, 1).wait_send()
    for j in range(2):
        rs_copy(RIGHT, K, j).wait_send()
        rs_copy(LEFT, K, 2 + j).wait_send()
    for off in (1, -1, 2, -2):
        dh_out(off).wait_send()
    for off in (3, -3, K):
        dh_on(1 if off > 0 else -1, off).wait_send()


def local(observations, returns, actions, w_input, w_middle, w_head, log_rate, copy_from, perturb):
    hbm = pl.BlockSpec(memory_space=pltpu.HBM)
    vmem = pl.BlockSpec(memory_space=pltpu.VMEM)
    smem = pl.BlockSpec(memory_space=pltpu.SMEM)
    V = pltpu.VMEM
    S = pltpu.SemaphoreType.DMA
    out = pl.pallas_call(
        kernel,
        out_shape=(
            pltpu.VMEM((8, D), BF16),
            pltpu.VMEM((64, D), BF16),
            pltpu.VMEM((ACT, 64), BF16),
            jax.ShapeDtypeStruct((1,), F32),
            jax.ShapeDtypeStruct((1,), F32),
        ),
        in_specs=[hbm, vmem, vmem, hbm, hbm, hbm, smem, smem, smem],
        out_specs=(vmem, vmem, vmem, smem, smem),
        scratch_shapes=[
            V((Q, ROWS, OBS), BF16),
            V((OBS, D), BF16),
            V((Z, 2, 2, 8, D), BF16),
            V((Z, 2, 2, ACT, 64), BF16),
            V((Z, Q, 64, QC), BF16),
            V((D, OBS), BF16),
            V((2, QC, BK), BF16),
            V((D, OBS), F32),
            V((D, D), BF16),
            V((D, D), BF16),
            V((QC, D), F32),
            V((QC, D), BF16),
            V((QC, D), BF16),
            V((128, QC), F32),
            V((QC, 128), BF16),
            V((32, QC), BF16),
            V((Q, 24, ROWS), F32),
            V((Q, 24, ROWS), F32),
            V((Q, 32, ROWS), BF16),
            V((Z, Q, 64, QC), F32),
            V((2, K, Q, 64, QC), BF16),
            V((2, K, Q, 64, QC), BF16),
            V((Z, 2, 2, 8, D), F32),
            V((Z, 2, 8, D), BF16),
            V((Z, 2, 8, D), BF16),
            V((2, K, 2, 8, D), BF16),
            V((2, K, 2, 8, D), BF16),
            V((2, 8, D), F32),
            V((8, D), BF16),
            V((8, D), BF16),
            V((8, D), BF16),
            V((8, D), BF16),
            V((Z, 24, QC), BF16),
            V((Q, 24, QC), F32),
            V((QC, 24), F32),
            V((Q, 64, QC), BF16),
            V((Q, 64, QC), BF16),
            V((Q, 64, QC), BF16),
            V((8, D), BF16),
            V((8, D), BF16),
            V((ACT, 64), BF16),
            V((ACT, 64), BF16),
            S((2, 2, K, 2)), S((2, 2, K, 2)),
            S((7,)), S((7,)),
            S((8,)), S((8,)),
            S((6, Q)), S((6, Q)),
            S((3,)), S((3,)),
            S((10,)), S((10,)),
            S((7,)), S((7,)),
            S((2, K, Q)), S((2, K, Q)),
            S((2, K, 2)), S((2, K, 2)),
            S((7,)), S((7,)),
            S((4,)),
        ],
        compiler_params=pltpu.CompilerParams(
            collective_id=0, has_side_effects=True, vmem_limit_bytes=60 * 1024 * 1024
        ),
    )(observations[0], returns, actions, w_input[0], w_middle[0], w_head[0].T, log_rate, copy_from, perturb)
    return out[0][None], out[1][None], out[2].T[None], out[3], out[4]


def solution(mesh):
    in_specs = (
        P("pop", "dp", None),
        P("pop", "dp"),
        P("pop", "dp"),
        P("pop", "dp", None),
        P("pop", "dp", None),
        P("pop", "dp", None),
        P(),
        P(),
        P(),
    )
    out_specs = (
        P("pop", "dp", None),
        P("pop", "dp", None),
        P("pop", "dp", None),
        P("pop"),
        P("pop"),
    )
    return jax.shard_map(local, mesh=mesh, in_specs=in_specs, out_specs=out_specs, check_vma=False)
```
